32 devices in a mesh: dp: 8 (over y, x, core), pencil: 4 (over z).
Axes of the slice: x: 2, y: 2, z: 4, core: 2. Of those that a mesh axis runs over, the one named last changes fastest.
Arguments:
- field: bfloat16 [8, 64, 64, 64, 128], P('dp', 'pencil'), may hold values from -6 to 6
- cotangent: bfloat16 [8, 64, 64, 64, 128], P('dp', 'pencil'), may hold values from -6 to 6
- w_spec: bfloat16 [16, 16, 16, 64, 128], P('dp', 'pencil'), may hold values from -6 to 6
- w_local: bfloat16 [64, 64], replicated, may hold values from -0.75 to 0.75
Outputs:
- grad_field: bfloat16 [8, 64, 64, 64, 128], P('dp', 'pencil')
- grad_w: float32 [16, 16, 16, 64, 128], P('dp', 'pencil')
The draws below stay inside these ranges and needn't reach their ends.
All inputs are finite; a program needn't handle non-finite values.
Results may differ from the reference program's by a relative error of at most 0.02.
Values may be sent and summed in bfloat16 or wider, within the bound.
A program may use at most 192 MiB of HBM per device.

```python
import math
import jax
import jax.numpy as jnp
from jax import lax

NX = 64
NY = 64
NZ = 128
CH = 64
MX = 16
MY = 16
MZ = 16
SAMPLES = 8


def block_levels(stream_key, shape, shards, smallest, largest):
    def one(dim, parts):
        draws = jax.random.uniform(jax.random.fold_in(jax.random.fold_in(stream_key, 6), dim), (parts,), jnp.float32, smallest / len(shards), largest / len(shards))
        return jnp.repeat(jnp.exp(draws), shape[dim] // parts).reshape((-1,) + (1,) * (len(shape) - dim - 1))

    level = one(*shards[0])
    for cut in shards[1:]:
        level = level * one(*cut)
    return level


def bell_draw(own_key, shape, scale, bound, cuts=(), kind=jnp.bfloat16):
    entries = jax.random.normal(own_key, shape, jnp.float32) * scale
    if len(cuts) > 0:
        entries = block_levels(own_key, shape, cuts, -0.22, 0.18) * entries
    return jnp.clip(entries, min=-bound, max=bound).astype(kind)


def setup_inputs(seed: int = 0) -> dict:
    arg_keys = jax.random.split(jax.random.key(seed), 5)
    field = bell_draw(arg_keys[0], (SAMPLES, NX, NY, CH, NZ), 1.0, 6.0, ((0, 8), (1, 4)))
    cotangent = bell_draw(arg_keys[1], (SAMPLES, NX, NY, CH, NZ), 1.0, 6.0, ((0, 8), (1, 4)))
    w_spec = bell_draw(arg_keys[2], (MX, MY, MZ, CH, 2 * CH), 1.0, 6.0, ((0, 8), (1, 4)))
    w_local = bell_draw(arg_keys[3], (CH, CH), CH ** -0.5, 0.75)
    return {"field": field, "cotangent": cotangent, "w_spec": w_spec, "w_local": w_local}


HIGHEST = lax.Precision.HIGHEST

def phase_pair(length, mode_count, signed):
    position = jnp.arange(length, dtype=jnp.int32)
    indices = jnp.arange(mode_count, dtype=jnp.int32)
    frequency = jnp.where(indices < mode_count // 2, indices, indices - mode_count) if signed else indices
    product = jnp.mod(position[:, None] * frequency[None, :], length).astype(jnp.float32)
    angles = product * (2.0 * math.pi / length)
    return (jnp.cos(angles), jnp.sin(angles))

def grid_tables():
    cos_x, sin_x = phase_pair(NX, MX, True)
    cos_y, sin_y = phase_pair(NY, MY, True)
    cos_z, sin_z = phase_pair(NZ, MZ, False)
    forward_z = jnp.concatenate([cos_z, -sin_z], 1).astype(jnp.bfloat16)
    weight_z = jnp.where(jnp.arange(MZ, dtype=jnp.int32) == 0, 1.0, 2.0).astype(jnp.float32) / (NX * NY * NZ)
    inverse_z = jnp.concatenate([cos_z * weight_z, -sin_z * weight_z], 1).T
    adjoint_z = jnp.concatenate([cos_z, -sin_z], 1).T
    spectrum_scale = jnp.concatenate([weight_z, weight_z])
    return (cos_x, sin_x, cos_y, sin_y, forward_z, inverse_z, adjoint_z, spectrum_scale)

def rotate_half(values):
    middle = values.shape[-1] // 2
    return jnp.concatenate([values[..., middle:], -values[..., :middle]], -1)

def along_y(values, cosines, sine_table, inverse):
    pattern = 'xjck,yj->xyck' if inverse else 'xyck,yj->xjck'
    factor = -1.0 if inverse else 1.0
    direct = jnp.einsum(pattern, values, cosines, precision=HIGHEST)
    turned = jnp.einsum(pattern, rotate_half(values), sine_table, precision=HIGHEST)
    return direct + factor * turned

def along_x(values, cosines, sine_table, inverse):
    pattern = 'jbck,xj->xbck' if inverse else 'xbck,xj->jbck'
    factor = -1.0 if inverse else 1.0
    direct = jnp.einsum(pattern, values, cosines, precision=HIGHEST)
    turned = jnp.einsum(pattern, rotate_half(values), sine_table, precision=HIGHEST)
    return direct + factor * turned

def z_forward(field_in, matrix):
    shape_in = field_in.shape
    product = jnp.dot(field_in.reshape(-1, shape_in[-1]), matrix, preferred_element_type=jnp.float32)
    return product.reshape(shape_in[:-1] + (matrix.shape[1],))

def z_back(values, matrix):
    shape_in = values.shape
    product = jnp.dot(values.reshape(-1, shape_in[-1]), matrix, precision=HIGHEST, preferred_element_type=jnp.float32)
    return product.reshape(shape_in[:-1] + (matrix.shape[1],))

def gelu_slope(pre):
    normal_cdf = 0.5 * (1.0 + lax.erf(pre * (1.0 / math.sqrt(2.0))))
    return normal_cdf + pre * jnp.exp(-0.5 * pre * pre) * (1.0 / math.sqrt(2.0 * math.pi))

def apply_modes(coeffs, weights):
    real_part = coeffs[..., :MZ]
    imag_part = coeffs[..., MZ:]
    from_real = jnp.einsum('abik,abkio->abok', real_part, weights, precision=HIGHEST)
    from_imag = jnp.einsum('abik,abkio->abok', imag_part, weights, precision=HIGHEST)
    out_real = from_real[:, :, :CH] - from_imag[:, :, CH:]
    out_imag = from_real[:, :, CH:] + from_imag[:, :, :CH]
    return jnp.concatenate([out_real, out_imag], -1)

def paired(g_modes):
    g_real = g_modes[..., :MZ]
    g_imag = g_modes[..., MZ:]
    return (jnp.concatenate([g_real, g_imag], -2), jnp.concatenate([g_imag, -g_real], -2))

def adjoint_modes(g_modes, weights):
    paired_one, paired_two = paired(g_modes)
    back_real = jnp.einsum('abkio,abok->abik', weights, paired_one, precision=HIGHEST)
    back_imag = jnp.einsum('abkio,abok->abik', weights, paired_two, precision=HIGHEST)
    return jnp.concatenate([back_real, back_imag], -1)

def mode_grads(u_modes, g_modes):
    paired_one, paired_two = paired(g_modes)
    from_real = jnp.einsum('abik,abok->abkio', u_modes[..., :MZ], paired_one, precision=HIGHEST)
    from_imag = jnp.einsum('abik,abok->abkio', u_modes[..., MZ:], paired_two, precision=HIGHEST)
    return from_real + from_imag

def reference(field, cotangent, w_spec, w_local):
    cos_x, sin_x, cos_y, sin_y, forward_z, inverse_z, adjoint_z, spectrum_scale = grid_tables()
    w_full = w_spec.astype(jnp.float32)
    w_bypass = w_local.astype(jnp.float32)

    def to_modes(field_in):
        sectioned = along_y(z_forward(field_in, forward_z), cos_y, sin_y, False)
        return along_x(sectioned, cos_x, sin_x, False)

    def to_grid(coeffs, matrix):
        sectioned = along_y(along_x(coeffs, cos_x, sin_x, True), cos_y, sin_y, True)
        return z_back(sectioned, matrix)

    def one_sample(accumulated, pair_in):
        sample, target = pair_in
        u_modes = lax.optimization_barrier(to_modes(sample).astype(jnp.bfloat16)).astype(jnp.float32)
        v_modes = apply_modes(u_modes, w_full)
        values = to_grid(v_modes, inverse_z)
        bypass = jnp.einsum('xycz,co->xyoz', sample.astype(jnp.float32), w_bypass, precision=HIGHEST)
        slope_in = (target.astype(jnp.float32) * gelu_slope(values + bypass)).astype(jnp.bfloat16)
        g_modes = lax.optimization_barrier((to_modes(slope_in) * spectrum_scale).astype(jnp.bfloat16)).astype(jnp.float32)
        accumulated = accumulated + mode_grads(u_modes, g_modes)
        back_modes = adjoint_modes(g_modes, w_full)
        spread = jnp.einsum('xyoz,co->xycz', slope_in.astype(jnp.float32), w_bypass, precision=HIGHEST)
        grad_sample = (to_grid(back_modes, adjoint_z) + spread).astype(jnp.bfloat16)
        return (accumulated, grad_sample)
    initial = jnp.zeros((MX, MY, MZ, CH, 2 * CH), jnp.float32)
    grad_w, grad_field = lax.scan(one_sample, initial, (field, cotangent))
    return (grad_field, grad_w)
```

```python
import math

import jax
import jax.numpy as jnp
import numpy as np
from jax import lax
from jax.experimental import pallas as pl
from jax.experimental.pallas import tpu as pltpu
from jax.sharding import PartitionSpec as P

BF16 = jnp.bfloat16
F32 = jnp.float32
ROWS = 16
PAIR = 2
YB = 4
VMEM = 67043328
MESH = pl.DeviceIdType.MESH


def waves(length, count, signed, positions=None):
    index = np.arange(count)
    freq = np.where(index < count // 2, index, index - count) if signed else index
    place = np.arange(length if positions is None else positions)
    angle = 2.0 * math.pi * ((place[:, None] * freq[None, :]) % length) / length
    return np.cos(angle), np.sin(angle)


def kron_rows(matrix):
    return np.kron(matrix, np.eye(ROWS))


def const(array):
    return jnp.asarray(np.asarray(array, np.float32), BF16)


def make_tables(nx, ny, nz, fold, packed, mx, my, mz, pencils):
    cx, sx = waves(nx, mx, True)
    cy, sy = waves(ny, my, True, ny // fold)
    cz, sz = waves(nz, mz, False)
    eye_t = np.eye(fold * packed)
    plain = np.concatenate([cz, -sz], 1)
    turned = np.concatenate([-sz, -cz], 1)
    z_fwd = np.concatenate([np.kron(eye_t, plain), np.kron(eye_t, turned)], 1)
    weight = np.where(np.arange(mz) == 0, 1.0, 2.0) / (nx * ny * nz)
    z_inv = np.kron(eye_t, np.concatenate([cz * weight, -sz * weight], 1).T)
    z_adj = np.kron(eye_t, plain.T)
    half = np.eye(mz)
    zero = np.zeros((mz, mz))
    block = np.block([[zero, -half], [half, zero]])
    turn_t = np.kron(eye_t, block)
    turn = np.kron(np.eye(2), turn_t)
    lanes = fold * packed * 2 * mz
    r_fwd = np.zeros((fold, packed, fold, 2 * mz, packed, fold, 2 * mz))
    r_inv = np.zeros((packed, fold, 2 * mz, fold, packed, fold, 2 * mz))
    for b in range(fold):
        for h in range(fold):
            angle = 2.0 * math.pi * ((b * h) % fold) / fold
            c, s = np.cos(angle) * half, np.sin(angle) * half
            for g in range(packed):
                r_fwd[b, g, h, :, g, b, :] = np.block([[c, -s], [s, c]])
                r_inv[g, b, :, b, g, h, :] = np.block([[c, s], [-s, c]])
    r_fwd = r_fwd.reshape(fold * lanes, lanes)
    r_inv = r_inv.reshape(lanes, fold * lanes)
    r_fwd = np.concatenate([r_fwd, r_fwd @ turn_t], 1)
    r_inv = np.concatenate([r_inv, r_inv @ np.kron(np.eye(fold), turn_t)], 1)
    y_fwd = np.concatenate([kron_rows(cy.T), kron_rows(sy.T)], 1)
    y_inv = np.concatenate([kron_rows(cy), -kron_rows(sy)], 1)
    own = nx // pencils
    x_fwd, x_inv = [], []
    for q in range(pencils):
        c, s = cx[q * own : (q + 1) * own], sx[q * own : (q + 1) * own]
        x_fwd.append(np.concatenate([kron_rows(c.T), kron_rows(s.T)], 1))
        x_inv.append(np.concatenate([kron_rows(c), -kron_rows(s)], 1))
    scale = np.tile(np.concatenate([weight, weight]), fold * packed)[None]
    return dict(
        z_fwd=const(z_fwd), z_inv=const(z_inv), z_adj=const(z_adj), turn=const(turn),
        y_fwd=const(y_fwd), y_inv=const(y_inv), r_fwd=const(r_fwd), r_inv=const(r_inv),
        x_fwd=const(np.stack(x_fwd)), x_inv=const(np.stack(x_inv)),
        scale=jnp.asarray(np.asarray(scale, np.float32)),
    )


def mm(a, b):
    return jnp.dot(a, b, preferred_element_type=F32)


def gelu_slope(pre):
    normal_cdf = 0.5 * (1.0 + lax.erf(pre * (1.0 / math.sqrt(2.0))))
    return normal_cdf + pre * jnp.exp(-0.5 * pre * pre) * (1.0 / math.sqrt(2.0 * math.pi))


def rows_of(index):
    return pl.ds(pl.multiple_of(index * ROWS, ROWS), ROWS)


def make_main(dims):
    pd, pp, jxl, jyl, mz, fold, packed, chunks = dims
    n = pd * pp
    nq = jyl // fold
    my = jyl * pp
    lanes = packed * fold * 2 * mz
    hm = fold * mz

    def kernel(
        field, cot, w, w_local, z_fwd, y_fwd, r_fwd, x_fwd, x_inv, turn, r_inv, y_inv, z_inv, scale,
        spread, columns, ucat, gcat,
        fbuf, cbuf, cols, sect, plain_in, turned_in, usend, vsend, bsend,
        urecv, vrecv, grecv, brecv, wbig, tbuf, obuf, xf, xi, mixer,
        fsem, csem, tsem, ssem, rsem, osem, colsem,
    ):
        xl, ny, ch, nz = fbuf.shape
        nyh = ny // fold
        pairs = xl // PAIR
        my_d, my_p = lax.axis_index("dp"), lax.axis_index("pencil")
        me = my_d * pp + my_p
        width = packed * ROWS

        barrier = pltpu.get_barrier_semaphore()

        def greet(i, carry):
            t = lax.rem(me + i, n)
            pl.semaphore_signal(
                barrier, inc=1, device_id=(t // pp, lax.rem(t, pp)), device_id_type=MESH
            )
            return carry

        lax.fori_loop(1, n, greet, 0)

        def piece(ref, g, i):
            return ref.at[pl.ds(i * PAIR, PAIR), :, pl.ds(pl.multiple_of(g * width, width), width), :]

        def load(src, dst, sem, g, i):
            return pltpu.make_async_copy(piece(src, g, i), piece(dst, g, i), sem.at[g, i])

        def start_all(src, dst, sem):
            def one(j, carry):
                load(src, dst, sem, j // pairs, lax.rem(j, pairs)).start()
                return carry

            lax.fori_loop(0, chunks * pairs, one, 0)

        x_tables = [
            pltpu.make_async_copy(x_fwd.at[my_p], xf, tsem.at[0]),
            pltpu.make_async_copy(x_inv.at[my_p], xi, tsem.at[1]),
        ]
        start_all(field, fbuf, fsem)
        for copy in x_tables:
            copy.start()
        start_all(cot, cbuf, csem)
        for copy in x_tables:
            copy.wait()

        def start_sends(source, recv, e, g):
            def one(i, carry):
                t = lax.rem(me + i, n)
                pltpu.make_async_remote_copy(
                    src_ref=source(t), dst_ref=recv.at[g, me],
                    send_sem=ssem.at[e, g], recv_sem=rsem.at[e, g],
                    device_id=(t // pp, lax.rem(t, pp)), device_id_type=MESH,
                ).start()
                return carry

            lax.fori_loop(1, n, one, 0)
            pltpu.make_async_copy(source(me), recv.at[g, me], rsem.at[e, g]).start()

        def wait_recv(recv, e, g):
            pltpu.make_async_copy(recv.at[g], recv.at[g], rsem.at[e, g]).wait()

        def wait_sends(recv, e):
            def one(g, carry):
                sent = recv.at[g, pl.ds(0, n - 1)]
                pltpu.make_async_copy(sent, sent, ssem.at[e, g]).wait()
                return carry

            lax.fori_loop(0, chunks, one, 0)

        def forward_pair(wides, x0):
            plain, turned = [], []
            for wide in wides:
                spectral = mm(wide, z_fwd[...]).astype(BF16)
                plain.append(spectral[:, :lanes])
                turned.append(spectral[:, lanes:])
            stacked = jnp.concatenate([jnp.concatenate(plain, 1), jnp.concatenate(turned, 1)], 0)
            out = mm(y_fwd[...], stacked).astype(BF16)
            for e in range(PAIR):
                sect[x0 + e] = out[:, e * lanes : (e + 1) * lanes]

        def forward_x(send, g):
            tiles = my // fold
            for q0 in range(0, tiles, 2):
                group = range(q0, min(q0 + 2, tiles))
                plain, turned = [], []
                for q in group:
                    rows = jnp.concatenate(
                        [
                            sect[:, (q * fold + b) * ROWS : (q * fold + b + 1) * ROWS, :].reshape(xl * ROWS, lanes)
                            for b in range(fold)
                        ],
                        1,
                    )
                    both = mm(rows, r_fwd[...]).astype(BF16)
                    plain.append(both[:, :lanes])
                    turned.append(both[:, lanes:])
                stacked = jnp.concatenate([jnp.concatenate(plain, 1), jnp.concatenate(turned, 1)], 0)
                got = mm(xf[...], stacked).astype(BF16)
                for e, q in enumerate(group):
                    for d in range(pd):
                        send[g, d * pp + q // nq, q % nq] = got[
                            d * jxl * ROWS : (d + 1) * jxl * ROWS, e * lanes : (e + 1) * lanes
                        ]

        def inverse_x(recv, g):
            tiles = my // fold
            for q0 in range(0, tiles, 2):
                group = range(q0, min(q0 + 2, tiles))
                rows = jnp.concatenate(
                    [
                        jnp.concatenate([recv[g, d * pp + q // nq, q % nq] for d in range(pd)], 0)
                        for q in group
                    ],
                    1,
                )
                size = rows.shape[1]
                turned = mm(rows, turn[:size, :size]).astype(BF16)
                got = mm(xi[...], jnp.concatenate([rows, turned], 0)).astype(BF16)
                for e, q in enumerate(group):
                    wide = mm(got[:, e * lanes : (e + 1) * lanes], r_inv[...]).astype(BF16)
                    for b in range(fold):
                        j = q * fold + b
                        at = slice(j * ROWS, (j + 1) * ROWS)
                        plain_in[:, at, :] = wide[:, b * lanes : (b + 1) * lanes].reshape(xl, ROWS, lanes)
                        turned_in[:, at, :] = wide[
                            :, (fold + b) * lanes : (fold + b + 1) * lanes
                        ].reshape(xl, ROWS, lanes)

        def inverse_y(x0):
            stacked = jnp.concatenate(
                [
                    jnp.concatenate([plain_in[x0 + e] for e in range(PAIR)], 1),
                    jnp.concatenate([turned_in[x0 + e] for e in range(PAIR)], 1),
                ],
                0,
            )
            return mm(y_inv[...], stacked).astype(BF16)

        def places(g):
            for gi in range(packed):
                for h in range(fold):
                    yield pl.ds(h * nyh, nyh), rows_of(g * packed + gi), (gi * fold + h) * nz

        def mix(matrix):
            tiled = jnp.concatenate([matrix] * YB, 1)
            owner = lax.broadcasted_iota(jnp.int32, (1, YB * ch), 1) // ch
            for b in range(YB):
                mixer[b * ch : (b + 1) * ch, :] = jnp.where(owner == b, tiled, 0.0).astype(BF16)

            def one(j, carry):
                x0 = (j // (ny // YB)) * PAIR
                ys = pl.ds(lax.rem(j, ny // YB) * YB, YB)
                wide = jnp.concatenate([fbuf[x0 + e, ys].reshape(YB * ch, nz) for e in range(PAIR)], 1)
                mixed = mm(mixer[...], wide).astype(BF16)
                for e in range(PAIR):
                    fbuf[x0 + e, ys] = mixed[:, e * nz : (e + 1) * nz].reshape(YB, ch, nz)
                return carry

            lax.fori_loop(0, pairs * (ny // YB), one, 0, unroll=2)

        def load_modes(recv, scaled):
            for jx in range(jxl):
                for ql in range(nq):
                    blocks = []
                    for s in range(pd):
                        for c in range(chunks):
                            at = slice(jx * ROWS, (jx + 1) * ROWS)
                            total = recv[c, s * pp, ql, at, :].astype(F32)
                            for q in range(1, pp):
                                total = total + recv[c, s * pp + q, ql, at, :].astype(F32)
                            blocks.append(total)
                    value = jnp.concatenate(blocks, 0)
                    if scaled:
                        value = value * scale[...]
                    flat = value.T
                    for s in range(pd):
                        for b in range(fold):
                            parts = []
                            for ri in range(2):
                                for c in range(chunks):
                                    for gi in range(packed):
                                        top = ((gi * fold + b) * 2 + ri) * mz
                                        left = (s * chunks + c) * ROWS
                                        if packed == 1 and c == 0:
                                            parts.append(flat[top : top + mz, left : left + ch])
                                        elif packed > 1:
                                            parts.append(flat[top : top + mz, left : left + ROWS])
                            low = s * hm + b * mz
                            tbuf[jx * nq + ql, low : low + mz, :] = jnp.concatenate(parts, 1)

        def store_modes(send):
            for jx in range(jxl):
                for ql in range(nq):
                    columns_of = []
                    for s in range(pd):
                        own = obuf[jx * nq + ql, s * hm : (s + 1) * hm, :]
                        if packed == 1:
                            columns_of.append(
                                jnp.concatenate(
                                    [
                                        own[b * mz : (b + 1) * mz, ri * ch : (ri + 1) * ch]
                                        for b in range(fold)
                                        for ri in range(2)
                                    ],
                                    0,
                                )
                            )
                        else:
                            for c in range(chunks):
                                columns_of.append(
                                    jnp.concatenate(
                                        [
                                            own[
                                                b * mz : (b + 1) * mz,
                                                ri * ch + (c * packed + gi) * ROWS : ri * ch + (c * packed + gi + 1) * ROWS,
                                            ]
                                            for gi in range(packed)
                                            for b in range(fold)
                                            for ri in range(2)
                                        ],
                                        0,
                                    )
                                )
                    back = jnp.concatenate(columns_of, 1).T.astype(BF16)
                    for s in range(pd):
                        for c in range(chunks):
                            low = (s * chunks + c) * ROWS
                            send[c, s, ql, jx * ROWS : (jx + 1) * ROWS, :] = back[low : low + ROWS, :]

        def each_mode(apply):
            def one(jq, carry):
                for r in range(hm):
                    own = tbuf[jq, pl.ds(r, pd, stride=hm), :]
                    obuf[jq, pl.ds(r, pd, stride=hm), :] = apply(jq * hm + r, own)
                return carry

            lax.fori_loop(0, jxl * nq, one, 0)

        def first(g, carry):
            def one(i, inner):
                load(field, fbuf, fsem, g, i).wait()
                wides = [
                    jnp.concatenate(
                        [fbuf[i * PAIR + e, ys, cs, :].reshape(nyh * ROWS, nz) for ys, cs, _ in places(g)], 1
                    )
                    for e in range(PAIR)
                ]
                forward_pair(wides, i * PAIR)
                return inner

            lax.fori_loop(0, pairs, one, 0)
            forward_x(usend, g)

            @pl.when(g == 0)
            def _():
                pl.semaphore_wait(barrier, n - 1)

            start_sends(lambda t: usend.at[g, t], urecv, 0, g)
            return carry

        lax.fori_loop(0, chunks, first, 0)

        sign = jnp.where(lax.broadcasted_iota(jnp.int32, (1, 2 * ch), 1) < ch, -1.0, 1.0).astype(F32)

        def prepare(m, carry):
            own = w[m].astype(F32)
            wbig[m, :ch, :] = w[m]
            wbig[m, ch:, :] = (pltpu.roll(own, ch, 1) * sign).astype(BF16)
            return carry

        lax.fori_loop(0, w.shape[0], prepare, 0, unroll=4)
        mix(w_local[...].astype(F32).T)

        def waits(recv, e):
            def one(g, carry):
                wait_recv(recv, e, g)
                return carry

            lax.fori_loop(0, chunks, one, 0)

        waits(urecv, 0)
        load_modes(urecv, False)

        def apply_one(m, own):
            ucat[m] = jnp.concatenate([own, pltpu.roll(own, ch, 1)], 0).astype(BF16)
            return mm(own.astype(BF16), wbig[m])

        each_mode(apply_one)
        store_modes(vsend)

        def send_v(g, carry):
            start_sends(lambda t: vsend.at[g, t // pp], vrecv, 1, g)
            return carry

        lax.fori_loop(0, chunks, send_v, 0)
        wait_sends(urecv, 0)

        def middle(g, carry):
            wait_recv(vrecv, 1, g)
            inverse_x(vrecv, g)

            def one(i, inner):
                load(cot, cbuf, csem, g, i).wait()
                col = inverse_y(i * PAIR)
                wides = []
                for e in range(PAIR):
                    x = i * PAIR + e
                    grid = mm(col[:, e * lanes : (e + 1) * lanes], z_inv[...])
                    pieces = []
                    for ys, cs, left in places(g):
                        pre = grid[:, left : left + nz].reshape(nyh, ROWS, nz) + fbuf[x, ys, cs, :].astype(F32)
                        slope = (cbuf[x, ys, cs, :].astype(F32) * gelu_slope(pre)).astype(BF16)
                        fbuf[x, ys, cs, :] = slope
                        pieces.append(slope.reshape(nyh * ROWS, nz))
                    wides.append(jnp.concatenate(pieces, 1))
                forward_pair(wides, i * PAIR)
                return inner

            lax.fori_loop(0, pairs, one, 0)
            forward_x(usend, g)
            start_sends(lambda t: usend.at[g, t], grecv, 2, g)
            return carry

        lax.fori_loop(0, chunks, middle, 0)

        mix(w_local[...].astype(F32))

        def spread_out(x):
            return pltpu.make_async_copy(fbuf.at[x], spread.at[x], osem.at[x])

        def put(x, carry):
            spread_out(x).start()
            return carry

        lax.fori_loop(0, xl, put, 0)

        waits(grecv, 2)
        load_modes(grecv, True)

        def adjoint_one(m, own):
            own = own.astype(BF16).astype(F32)
            gcat[m] = jnp.concatenate([own, pltpu.roll(own, ch, 1) * -sign], 0).astype(BF16)
            return lax.dot_general(
                own.astype(BF16), wbig[m], (((1,), (1,)), ((), ())), preferred_element_type=F32
            )

        each_mode(adjoint_one)
        store_modes(bsend)

        def send_b(g, carry):
            start_sends(lambda t: bsend.at[g, t // pp], brecv, 3, g)
            return carry

        lax.fori_loop(0, chunks, send_b, 0)

        def cols_out(g, x):
            return pltpu.make_async_copy(cols.at[g, x], columns.at[g, x], colsem.at[g, x])

        def last(g, carry):
            wait_recv(brecv, 3, g)
            inverse_x(brecv, g)

            def one(i, inner):
                col = inverse_y(i * PAIR)
                for e in range(PAIR):
                    cols[g, i * PAIR + e] = col[:, e * lanes : (e + 1) * lanes]
                    cols_out(g, i * PAIR + e).start()
                return inner

            lax.fori_loop(0, pairs, one, 0)
            return carry

        lax.fori_loop(0, chunks, last, 0)
        wait_sends(vrecv, 1)
        wait_sends(grecv, 2)
        wait_sends(brecv, 3)

        def finish(x, carry):
            spread_out(x).wait()
            for g in range(chunks):
                cols_out(g, x).wait()
            return carry

        lax.fori_loop(0, xl, finish, 0)

    return kernel


def make_last(fold, packed, chunks):
    def kernel(spread, columns, z_adj, ucat, gcat, grad, grad_w):
        xs, ny, ch, nz = spread.shape
        nyh = ny // fold
        for x in range(xs):
            for g in range(chunks):
                grid = mm(columns[g, x], z_adj[...])
                for gi in range(packed):
                    for h in range(fold):
                        left = (gi * fold + h) * nz
                        ys = slice(h * nyh, (h + 1) * nyh)
                        cs = slice((g * packed + gi) * ROWS, (g * packed + gi + 1) * ROWS)
                        value = grid[:, left : left + nz].reshape(nyh, ROWS, nz)
                        grad[x, ys, cs, :] = (value + spread[x, ys, cs, :].astype(F32)).astype(BF16)
        for m in range(grad_w.shape[0]):
            grad_w[m] = lax.dot_general(
                ucat[m], gcat[m], (((0,), (0,)), ((), ())), preferred_element_type=F32
            )[:ch]

    return kernel


def whole(array):
    return pl.BlockSpec(array.shape, lambda i, n=len(array.shape): (0,) * n)


def solution(mesh):
    pd, pp = mesh.shape["dp"], mesh.shape["pencil"]

    def body(field, cotangent, w_spec, w_local):
        sample, target = field[0], cotangent[0]
        xl, ny, ch, nz = sample.shape
        jxl, jyl, mz = w_spec.shape[:3]
        mx, my = jxl * pd, jyl * pp
        groups = ch // ROWS
        fold = math.gcd(jyl, groups)
        packed = groups // fold
        chunks = groups // packed
        lanes = groups * 2 * mz
        nq = jyl // fold
        n = pd * pp
        modes = jxl * jyl * mz
        pairs = xl // PAIR
        nyh = ny // fold
        t = make_tables(xl * pp, ny, nz, fold, packed, mx, my, mz, pp)
        weights = w_spec.reshape(modes, ch, 2 * ch)
        hbm = pl.BlockSpec(memory_space=pl.ANY)
        vmem = pl.BlockSpec(memory_space=pltpu.VMEM)
        names = ("z_fwd", "y_fwd", "r_fwd", "x_fwd", "x_inv", "turn", "r_inv", "y_inv", "z_inv", "scale")
        tables = [t[name] for name in names]
        table_specs = [hbm if name in ("x_fwd", "x_inv") else vmem for name in names]
        block = (nq, jxl * ROWS, lanes)
        part = pltpu.VMEM((chunks, n) + block, BF16)
        mode_part = pltpu.VMEM((chunks, pd) + block, BF16)
        section = pltpu.VMEM((xl, my * ROWS, lanes), BF16)
        grid_buf = pltpu.VMEM(sample.shape, BF16)
        by_mode = pltpu.VMEM((jxl * nq, pd * fold * mz, 2 * ch), F32)
        dma = pltpu.SemaphoreType.DMA
        dims = (pd, pp, jxl, jyl, mz, fold, packed, chunks)
        cat = jax.ShapeDtypeStruct((modes, 2 * pd, 2 * ch), BF16)
        spread, columns, ucat, gcat = pl.pallas_call(
            make_main(dims),
            in_specs=[hbm, hbm, vmem, vmem] + table_specs,
            out_specs=[hbm, hbm, vmem, vmem],
            out_shape=[
                jax.ShapeDtypeStruct(sample.shape, BF16),
                jax.ShapeDtypeStruct((chunks, xl, nyh * ROWS, lanes), BF16),
                cat,
                cat,
            ],
            scratch_shapes=[
                grid_buf, grid_buf,
                pltpu.VMEM((chunks, xl, nyh * ROWS, lanes), BF16),
                section, section, section,
                part, mode_part, mode_part,
                part, part, part, part,
                pltpu.VMEM((modes, 2 * ch, 2 * ch), BF16),
                by_mode, by_mode,
                pltpu.VMEM(t["x_fwd"].shape[1:], BF16),
                pltpu.VMEM(t["x_inv"].shape[1:], BF16),
                pltpu.VMEM((YB * ch, YB * ch), BF16),
                dma((chunks, pairs)), dma((chunks, pairs)), dma((2,)),
                dma((4, chunks)), dma((4, chunks)), dma((xl,)), dma((chunks, xl)),
            ],
            compiler_params=pltpu.CompilerParams(
                collective_id=0, has_side_effects=True, vmem_limit_bytes=VMEM
            ),
        )(sample, target, weights, w_local, *tables)

        per = modes // pairs
        grad, grad_w = pl.pallas_call(
            make_last(fold, packed, chunks),
            grid=(pairs,),
            in_specs=[
                pl.BlockSpec((PAIR, ny, ch, nz), lambda i: (i, 0, 0, 0)),
                pl.BlockSpec((chunks, PAIR, nyh * ROWS, lanes), lambda i: (0, i, 0, 0)),
                whole(t["z_adj"]),
                pl.BlockSpec((per, 2 * pd, 2 * ch), lambda i: (i, 0, 0)),
                pl.BlockSpec((per, 2 * pd, 2 * ch), lambda i: (i, 0, 0)),
            ],
            out_specs=[
                pl.BlockSpec((PAIR, ny, ch, nz), lambda i: (i, 0, 0, 0)),
                pl.BlockSpec((per, ch, 2 * ch), lambda i: (i, 0, 0)),
            ],
            out_shape=[
                jax.ShapeDtypeStruct(sample.shape, BF16),
                jax.ShapeDtypeStruct((modes, ch, 2 * ch), F32),
            ],
            compiler_params=pltpu.CompilerParams(
                dimension_semantics=("arbitrary",), vmem_limit_bytes=VMEM
            ),
        )(spread, columns, t["z_adj"], ucat, gcat)
        return grad[None], grad_w.reshape(w_spec.shape)

    grid_spec = P("dp", "pencil", None, None, None)
    return jax.shard_map(
        body,
        mesh=mesh,
        in_specs=(grid_spec, grid_spec, grid_spec, P()),
        out_specs=(grid_spec, grid_spec),
        check_vma=False,
    )
```

```python
import math

import jax
import jax.numpy as jnp
import numpy as np
from jax import lax
from jax.experimental import pallas as pl
from jax.experimental.pallas import tpu as pltpu
from jax.sharding import PartitionSpec as P

BF16 = jnp.bfloat16
F32 = jnp.float32
ROWS = 16
PAIR = 2
YB = 4
BATCH = 8
VMEM = 67043328
MESH = pl.DeviceIdType.MESH


def waves(length, count, signed, positions=None):
    index = np.arange(count)
    freq = np.where(index < count // 2, index, index - count) if signed else index
    place = np.arange(length if positions is None else positions)
    angle = 2.0 * math.pi * ((place[:, None] * freq[None, :]) % length) / length
    return np.cos(angle), np.sin(angle)


def const(array):
    return jnp.asarray(np.asarray(array, np.float32), BF16)


def make_tables(nx, ny, nz, fold, packed, mx, my, mz, pencils):
    cx, sx = waves(nx, mx, True)
    cy, sy = waves(ny, my, True, ny // fold)
    cz, sz = waves(nz, mz, False)
    eye_t = np.eye(fold * packed)
    plain = np.concatenate([cz, -sz], 1)
    turned = np.concatenate([-sz, -cz], 1)
    z_fwd = np.concatenate([np.kron(eye_t, plain), np.kron(eye_t, turned)], 1)
    weight = np.where(np.arange(mz) == 0, 1.0, 2.0) / (nx * ny * nz)
    z_inv = np.kron(eye_t, np.concatenate([cz * weight, -sz * weight], 1).T)
    z_adj = np.kron(eye_t, plain.T)
    half = np.eye(mz)
    zero = np.zeros((mz, mz))
    block = np.block([[zero, -half], [half, zero]])
    turn_t = np.kron(eye_t, block)
    turn = np.kron(np.eye(2), turn_t)
    lanes = fold * packed * 2 * mz
    r_fwd = np.zeros((fold, packed, fold, 2 * mz, packed, fold, 2 * mz))
    r_inv = np.zeros((packed, fold, 2 * mz, fold, packed, fold, 2 * mz))
    for b in range(fold):
        for h in range(fold):
            angle = 2.0 * math.pi * ((b * h) % fold) / fold
            c, s = np.cos(angle) * half, np.sin(angle) * half
            for g in range(packed):
                r_fwd[b, g, h, :, g, b, :] = np.block([[c, -s], [s, c]])
                r_inv[g, b, :, b, g, h, :] = np.block([[c, s], [-s, c]])
    r_fwd = r_fwd.reshape(fold * lanes, lanes)
    r_inv = r_inv.reshape(lanes, fold * lanes)
    r_fwd = np.concatenate([r_fwd, r_fwd @ turn_t], 1)
    r_inv = np.concatenate([r_inv, r_inv @ np.kron(np.eye(fold), turn_t)], 1)
    own = nx // pencils
    cx, sx = cx.reshape(pencils, own, mx), sx.reshape(pencils, own, mx)
    y_fwd = np.stack([cy.T, sy.T])
    y_inv = np.stack([cy, -sy])
    x_fwd = np.stack([cx.transpose(0, 2, 1), sx.transpose(0, 2, 1)], 1)
    x_inv = np.stack([cx, -sx], 1)
    scale = np.tile(np.concatenate([weight, weight]), fold * packed)[None]
    return dict(
        z_fwd=const(z_fwd), z_inv=const(z_inv), z_adj=const(z_adj), turn=const(turn),
        y_fwd=const(y_fwd), y_inv=const(y_inv), r_fwd=const(r_fwd), r_inv=const(r_inv),
        x_fwd=const(x_fwd), x_inv=const(x_inv),
        scale=jnp.asarray(np.asarray(scale, np.float32)),
    )


def mm(a, b):
    return jnp.dot(a, b, preferred_element_type=F32)


def gelu_slope(pre):
    normal_cdf = 0.5 * (1.0 + lax.erf(pre * (1.0 / math.sqrt(2.0))))
    return normal_cdf + pre * jnp.exp(-0.5 * pre * pre) * (1.0 / math.sqrt(2.0 * math.pi))


def expand(small):
    a, b = small.shape
    shift = ROWS.bit_length() - 1

    def iota(shape, axis):
        return lax.broadcasted_iota(jnp.int32, shape, axis)

    def same(left, right):
        return jnp.where(left == right, 1.0, 0.0).astype(BF16)

    tall, wide, full = (a * ROWS, a), (b, b * ROWS), (a * ROWS, b * ROWS)
    up = same(iota(tall, 0) >> shift, iota(tall, 1))
    out = same(iota(wide, 0), iota(wide, 1) >> shift)
    value = mm(mm(up, small).astype(BF16), out)
    return jnp.where((iota(full, 0) & (ROWS - 1)) == (iota(full, 1) & (ROWS - 1)), value, 0.0).astype(BF16)


def rows_of(index):
    return pl.ds(pl.multiple_of(index * ROWS, ROWS), ROWS)


def make_main(dims):
    pd, pp, jxl, jyl, mz, fold, packed, chunks = dims
    n = pd * pp
    nq = jyl // fold
    my = jyl * pp
    lanes = packed * fold * 2 * mz
    hm = fold * mz

    def kernel(
        field, cot, w, w_local, z_fwd, y_small, r_fwd, x_small, x_back, turn, r_inv, y_back, z_inv, scale,
        spread, columns, ucat, gcat,
        fbuf, cbuf, cols, sect, plain_in, turned_in, usend, vsend, bsend,
        urecv, vrecv, grecv, brecv, wbig, tbuf, obuf, xf, xi, y_fwd, y_inv, mixer, staged, cstage,
        fsem, csem, ssem, rsem, osem, colsem,
    ):
        xl, ny, ch, nz = fbuf.shape
        nyh = ny // fold
        pairs = xl // PAIR
        batch = staged.shape[1] // lanes
        batches = xl // batch
        my_d, my_p = lax.axis_index("dp"), lax.axis_index("pencil")
        me = my_d * pp + my_p
        width = packed * ROWS

        barrier = pltpu.get_barrier_semaphore()

        def greet(i, carry):
            t = lax.rem(me + i, n)
            pl.semaphore_signal(
                barrier, inc=1, device_id=(lax.div(t, pp), lax.rem(t, pp)), device_id_type=MESH
            )
            return carry

        lax.fori_loop(1, n, greet, 0)

        def piece(ref, g, i):
            return ref.at[pl.ds(i * PAIR, PAIR), :, pl.ds(pl.multiple_of(g * width, width), width), :]

        def load(src, dst, sem, g, i):
            return pltpu.make_async_copy(piece(src, g, i), piece(dst, g, i), sem.at[g, i])

        def start_all(src, dst, sem):
            def one(j, carry):
                load(src, dst, sem, j // pairs, lax.rem(j, pairs)).start()
                return carry

            lax.fori_loop(0, chunks * pairs, one, 0)

        start_all(field, fbuf, fsem)
        start_all(cot, cbuf, csem)
        for table, small in ((xf, x_small.at[my_p]), (xi, x_back.at[my_p]), (y_fwd, y_small), (y_inv, y_back)):
            half = table.shape[1] // 2
            for part in range(2):
                table[:, part * half : (part + 1) * half] = expand(small[part])

        def start_sends(source, recv, e, g):
            def one(i, carry):
                t = lax.rem(me + i, n)
                pltpu.make_async_remote_copy(
                    src_ref=source(t), dst_ref=recv.at[g, me],
                    send_sem=ssem.at[e, g], recv_sem=rsem.at[e, g],
                    device_id=(lax.div(t, pp), lax.rem(t, pp)), device_id_type=MESH,
                ).start()
                return carry

            lax.fori_loop(1, n, one, 0, unroll=8)
            pltpu.make_async_copy(source(me), recv.at[g, me], rsem.at[e, g]).start()

        def wait_recv(recv, e, g):
            pltpu.make_async_copy(recv.at[g], recv.at[g], rsem.at[e, g]).wait()

        def wait_sends(recv, e):
            def one(g, carry):
                sent = recv.at[g, pl.ds(0, n - 1)]
                pltpu.make_async_copy(sent, sent, ssem.at[e, g]).wait()
                return carry

            lax.fori_loop(0, chunks, one, 0)

        def forward_z(wide, e):
            spectral = mm(wide, z_fwd[...]).astype(BF16)
            rows = nyh * ROWS
            staged[:rows, e * lanes : (e + 1) * lanes] = spectral[:, :lanes]
            staged[rows:, e * lanes : (e + 1) * lanes] = spectral[:, lanes:]

        def forward_y(x0):
            for k in range(0, batch, PAIR):
                out = mm(y_fwd[...], staged[:, k * lanes : (k + PAIR) * lanes]).astype(BF16)
                for e in range(PAIR):
                    sect[x0 + k + e] = out[:, e * lanes : (e + 1) * lanes]

        def forward_x(send, g):
            tiles = my // fold
            for q0 in range(0, tiles, 2):
                group = range(q0, min(q0 + 2, tiles))
                plain, turned = [], []
                for q in group:
                    rows = jnp.concatenate(
                        [
                            sect[:, (q * fold + b) * ROWS : (q * fold + b + 1) * ROWS, :].reshape(xl * ROWS, lanes)
                            for b in range(fold)
                        ],
                        1,
                    )
                    both = mm(rows, r_fwd[...]).astype(BF16)
                    plain.append(both[:, :lanes])
                    turned.append(both[:, lanes:])
                stacked = jnp.concatenate([jnp.concatenate(plain, 1), jnp.concatenate(turned, 1)], 0)
                got = mm(xf[...], stacked).astype(BF16)
                for e, q in enumerate(group):
                    for d in range(pd):
                        send[g, d * pp + q // nq, q % nq] = got[
                            d * jxl * ROWS : (d + 1) * jxl * ROWS, e * lanes : (e + 1) * lanes
                        ]

        def inverse_x(recv, g):
            tiles = my // fold
            for q0 in range(0, tiles, 2):
                group = range(q0, min(q0 + 2, tiles))
                rows = jnp.concatenate(
                    [
                        jnp.concatenate([recv[g, d * pp + q // nq, q % nq] for d in range(pd)], 0)
                        for q in group
                    ],
                    1,
                )
                size = rows.shape[1]
                turned = mm(rows, turn[:size, :size]).astype(BF16)
                got = mm(xi[...], jnp.concatenate([rows, turned], 0)).astype(BF16)
                for e, q in enumerate(group):
                    wide = mm(got[:, e * lanes : (e + 1) * lanes], r_inv[...]).astype(BF16)
                    for b in range(fold):
                        j = q * fold + b
                        at = slice(j * ROWS, (j + 1) * ROWS)
                        plain_in[:, at, :] = wide[:, b * lanes : (b + 1) * lanes].reshape(xl, ROWS, lanes)
                        turned_in[:, at, :] = wide[
                            :, (fold + b) * lanes : (fold + b + 1) * lanes
                        ].reshape(xl, ROWS, lanes)

        def inverse_y(x0):
            stacked = jnp.concatenate(
                [
                    jnp.concatenate([plain_in[x0 + e] for e in range(PAIR)], 1),
                    jnp.concatenate([turned_in[x0 + e] for e in range(PAIR)], 1),
                ],
                0,
            )
            return mm(y_inv[...], stacked).astype(BF16)

        def places(g):
            for gi in range(packed):
                for h in range(fold):
                    yield pl.ds(h * nyh, nyh), rows_of(g * packed + gi), (gi * fold + h) * nz

        def mix(matrix):
            tiled = jnp.concatenate([matrix] * YB, 1)
            owner = lax.broadcasted_iota(jnp.int32, (1, YB * ch), 1) // ch
            for b in range(YB):
                mixer[b * ch : (b + 1) * ch, :] = jnp.where(owner == b, tiled, 0.0).astype(BF16)

            steps = math.gcd(ny // YB, 16)
            per = ny // YB // steps

            def one(j, carry):
                x0 = (j // per) * PAIR
                y0 = lax.rem(j, per) * (YB * steps)
                for u in range(steps):
                    ys = pl.ds(y0 + u * YB, YB)
                    wide = jnp.concatenate([fbuf[x0 + e, ys].reshape(YB * ch, nz) for e in range(PAIR)], 1)
                    mixed = mm(mixer[...], wide).astype(BF16)
                    for e in range(PAIR):
                        fbuf[x0 + e, ys] = mixed[:, e * nz : (e + 1) * nz].reshape(YB, ch, nz)
                return carry

            lax.fori_loop(0, pairs * per, one, 0)

        def load_modes(recv, scaled):
            for jx in range(jxl):
                for ql in range(nq):
                    blocks = []
                    for s in range(pd):
                        for c in range(chunks):
                            at = slice(jx * ROWS, (jx + 1) * ROWS)
                            total = recv[c, s * pp, ql, at, :].astype(F32)
                            for q in range(1, pp):
                                total = total + recv[c, s * pp + q, ql, at, :].astype(F32)
                            blocks.append(total)
                    value = jnp.concatenate(blocks, 0)
                    if scaled:
                        value = value * scale[...]
                    flat = value.T
                    for s in range(pd):
                        for b in range(fold):
                            parts = []
                            for ri in range(2):
                                for c in range(chunks):
                                    for gi in range(packed):
                                        top = ((gi * fold + b) * 2 + ri) * mz
                                        left = (s * chunks + c) * ROWS
                                        if packed == 1 and c == 0:
                                            parts.append(flat[top : top + mz, left : left + ch])
                                        elif packed > 1:
                                            parts.append(flat[top : top + mz, left : left + ROWS])
                            low = s * hm + b * mz
                            tbuf[jx * nq + ql, low : low + mz, :] = jnp.concatenate(parts, 1)

        def store_modes(send):
            for jx in range(jxl):
                for ql in range(nq):
                    columns_of = []
                    for s in range(pd):
                        own = obuf[jx * nq + ql, s * hm : (s + 1) * hm, :]
                        if packed == 1:
                            columns_of.append(
                                jnp.concatenate(
                                    [
                                        own[b * mz : (b + 1) * mz, ri * ch : (ri + 1) * ch]
                                        for b in range(fold)
                                        for ri in range(2)
                                    ],
                                    0,
                                )
                            )
                        else:
                            for c in range(chunks):
                                columns_of.append(
                                    jnp.concatenate(
                                        [
                                            own[
                                                b * mz : (b + 1) * mz,
                                                ri * ch + (c * packed + gi) * ROWS : ri * ch + (c * packed + gi + 1) * ROWS,
                                            ]
                                            for gi in range(packed)
                                            for b in range(fold)
                                            for ri in range(2)
                                        ],
                                        0,
                                    )
                                )
                    back = jnp.concatenate(columns_of, 1).T.astype(BF16)
                    for s in range(pd):
                        for c in range(chunks):
                            low = (s * chunks + c) * ROWS
                            send[c, s, ql, jx * ROWS : (jx + 1) * ROWS, :] = back[low : low + ROWS, :]

        def each_mode(apply):
            def one(jq, carry):
                for r in range(hm):
                    own = tbuf[jq, pl.ds(r, pd, stride=hm), :]
                    obuf[jq, pl.ds(r, pd, stride=hm), :] = apply(jq * hm + r, own)
                return carry

            lax.fori_loop(0, jxl * nq, one, 0)

        def first(g, carry):
            def one(i, inner):
                x0 = i * batch
                for k in range(batch // PAIR):
                    load(field, fbuf, fsem, g, i * (batch // PAIR) + k).wait()
                for e in range(batch):
                    forward_z(
                        jnp.concatenate(
                            [fbuf[x0 + e, ys, cs, :].reshape(nyh * ROWS, nz) for ys, cs, _ in places(g)], 1
                        ),
                        e,
                    )
                forward_y(x0)
                return inner

            lax.fori_loop(0, batches, one, 0)
            forward_x(usend, g)

            @pl.when(g == 0)
            def _():
                pl.semaphore_wait(barrier, n - 1)

            start_sends(lambda t: usend.at[g, t], urecv, 0, g)
            return carry

        lax.fori_loop(0, chunks, first, 0)

        sign = jnp.where(lax.broadcasted_iota(jnp.int32, (1, 2 * ch), 1) < ch, -1.0, 1.0).astype(F32)

        def prepare(m, carry):
            own = w[m].astype(F32)
            wbig[m, :ch, :] = w[m]
            wbig[m, ch:, :] = (pltpu.roll(own, ch, 1) * sign).astype(BF16)
            return carry

        lax.fori_loop(0, w.shape[0], prepare, 0, unroll=4)
        mix(w_local[...].astype(F32).T)

        def waits(recv, e):
            def one(g, carry):
                wait_recv(recv, e, g)
                return carry

            lax.fori_loop(0, chunks, one, 0)

        waits(urecv, 0)
        load_modes(urecv, False)

        def apply_one(m, own):
            ucat[m] = jnp.concatenate([own, pltpu.roll(own, ch, 1)], 0).astype(BF16)
            return mm(own.astype(BF16), wbig[m])

        each_mode(apply_one)
        store_modes(vsend)

        def send_v(g, carry):
            start_sends(lambda t: vsend.at[g, lax.div(t, pp)], vrecv, 1, g)
            return carry

        lax.fori_loop(0, chunks, send_v, 0)
        wait_sends(urecv, 0)

        def middle(g, carry):
            wait_recv(vrecv, 1, g)
            inverse_x(vrecv, g)

            def one(i, inner):
                x0 = i * batch
                for k in range(batch // PAIR):
                    load(cot, cbuf, csem, g, i * (batch // PAIR) + k).wait()
                for k in range(0, batch, PAIR):
                    cstage[:, k * lanes : (k + PAIR) * lanes] = inverse_y(x0 + k)
                for e in range(batch):
                    grid = mm(cstage[:, e * lanes : (e + 1) * lanes], z_inv[...])
                    pieces = []
                    for ys, cs, left in places(g):
                        pre = grid[:, left : left + nz].reshape(nyh, ROWS, nz) + fbuf[x0 + e, ys, cs, :].astype(F32)
                        slope = (cbuf[x0 + e, ys, cs, :].astype(F32) * gelu_slope(pre)).astype(BF16)
                        fbuf[x0 + e, ys, cs, :] = slope
                        pieces.append(slope.reshape(nyh * ROWS, nz))
                    forward_z(jnp.concatenate(pieces, 1), e)
                forward_y(x0)
                return inner

            lax.fori_loop(0, batches, one, 0)
            forward_x(usend, g)
            start_sends(lambda t: usend.at[g, t], grecv, 2, g)
            return carry

        lax.fori_loop(0, chunks, middle, 0)

        mix(w_local[...].astype(F32))

        def spread_out(x):
            return pltpu.make_async_copy(fbuf.at[x], spread.at[x], osem.at[x])

        def put(x, carry):
            spread_out(x).start()
            return carry

        lax.fori_loop(0, xl, put, 0)

        waits(grecv, 2)
        load_modes(grecv, True)

        def adjoint_one(m, own):
            own = own.astype(BF16).astype(F32)
            gcat[m] = jnp.concatenate([own, pltpu.roll(own, ch, 1) * -sign], 0).astype(BF16)
            return lax.dot_general(
                own.astype(BF16), wbig[m], (((1,), (1,)), ((), ())), preferred_element_type=F32
            )

        each_mode(adjoint_one)
        store_modes(bsend)

        def send_b(g, carry):
            start_sends(lambda t: bsend.at[g, lax.div(t, pp)], brecv, 3, g)
            return carry

        lax.fori_loop(0, chunks, send_b, 0)

        def cols_out(g, x):
            return pltpu.make_async_copy(cols.at[g, x], columns.at[g, x], colsem.at[g, x])

        def last(g, carry):
            wait_recv(brecv, 3, g)
            inverse_x(brecv, g)

            def one(i, inner):
                for k in range(0, batch, PAIR):
                    x0 = i * batch + k
                    col = inverse_y(x0)
                    for e in range(PAIR):
                        cols[g, x0 + e] = col[:, e * lanes : (e + 1) * lanes]
                return inner

            lax.fori_loop(0, batches, one, 0)

            def out(x, inner):
                cols_out(g, x).start()
                return inner

            lax.fori_loop(0, xl, out, 0)
            return carry

        lax.fori_loop(0, chunks, last, 0)
        wait_sends(vrecv, 1)
        wait_sends(grecv, 2)
        wait_sends(brecv, 3)

        def finish(x, carry):
            spread_out(x).wait()
            for g in range(chunks):
                cols_out(g, x).wait()
            return carry

        lax.fori_loop(0, xl, finish, 0)

    return kernel


def make_last(fold, packed, chunks):
    def kernel(spread, columns, z_adj, ucat, gcat, grad, grad_w):
        xs, ny, ch, nz = spread.shape
        nyh = ny // fold
        for x in range(xs):
            for g in range(chunks):
                grid = mm(columns[g, x], z_adj[...])
                for gi in range(packed):
                    for h in range(fold):
                        left = (gi * fold + h) * nz
                        ys = slice(h * nyh, (h + 1) * nyh)
                        cs = slice((g * packed + gi) * ROWS, (g * packed + gi + 1) * ROWS)
                        value = grid[:, left : left + nz].reshape(nyh, ROWS, nz)
                        grad[x, ys, cs, :] = (value + spread[x, ys, cs, :].astype(F32)).astype(BF16)
        for m in range(grad_w.shape[0]):
            grad_w[m] = lax.dot_general(
                ucat[m], gcat[m], (((0,), (0,)), ((), ())), preferred_element_type=F32
            )[:ch]

    return kernel


def whole(array):
    return pl.BlockSpec(array.shape, lambda i, n=len(array.shape): (0,) * n)


def solution(mesh):
    pd, pp = mesh.shape["dp"], mesh.shape["pencil"]

    def body(field, cotangent, w_spec, w_local):
        sample, target = field[0], cotangent[0]
        xl, ny, ch, nz = sample.shape
        jxl, jyl, mz = w_spec.shape[:3]
        mx, my = jxl * pd, jyl * pp
        groups = ch // ROWS
        fold = math.gcd(jyl, groups)
        packed = groups // fold
        chunks = groups // packed
        lanes = groups * 2 * mz
        nq = jyl // fold
        n = pd * pp
        modes = jxl * jyl * mz
        pairs = xl // PAIR
        nyh = ny // fold
        t = make_tables(xl * pp, ny, nz, fold, packed, mx, my, mz, pp)
        weights = w_spec.reshape(modes, ch, 2 * ch)
        hbm = pl.BlockSpec(memory_space=pl.ANY)
        vmem = pl.BlockSpec(memory_space=pltpu.VMEM)
        names = ("z_fwd", "y_fwd", "r_fwd", "x_fwd", "x_inv", "turn", "r_inv", "y_inv", "z_inv", "scale")
        tables = [t[name] for name in names]
        table_specs = [vmem] * len(names)
        batch = math.gcd(xl, BATCH)
        block = (nq, jxl * ROWS, lanes)
        part = pltpu.VMEM((chunks, n) + block, BF16)
        mode_part = pltpu.VMEM((chunks, pd) + block, BF16)
        section = pltpu.VMEM((xl, my * ROWS, lanes), BF16)
        grid_buf = pltpu.VMEM(sample.shape, BF16)
        by_mode = pltpu.VMEM((jxl * nq, pd * fold * mz, 2 * ch), F32)
        dma = pltpu.SemaphoreType.DMA
        dims = (pd, pp, jxl, jyl, mz, fold, packed, chunks)
        cat = jax.ShapeDtypeStruct((modes, 2 * pd, 2 * ch), BF16)
        spread, columns, ucat, gcat = pl.pallas_call(
            make_main(dims),
            in_specs=[hbm, hbm, vmem, vmem] + table_specs,
            out_specs=[hbm, hbm, vmem, vmem],
            out_shape=[
                jax.ShapeDtypeStruct(sample.shape, BF16),
                jax.ShapeDtypeStruct((chunks, xl, nyh * ROWS, lanes), BF16),
                cat,
                cat,
            ],
            scratch_shapes=[
                grid_buf, grid_buf,
                pltpu.VMEM((chunks, xl, nyh * ROWS, lanes), BF16),
                section, section, section,
                part, mode_part, mode_part,
                part, part, part, part,
                pltpu.VMEM((modes, 2 * ch, 2 * ch), BF16),
                by_mode, by_mode,
                pltpu.VMEM((mx * ROWS, 2 * xl * ROWS), BF16),
                pltpu.VMEM((xl * ROWS, 2 * mx * ROWS), BF16),
                pltpu.VMEM((my * ROWS, 2 * nyh * ROWS), BF16),
                pltpu.VMEM((nyh * ROWS, 2 * my * ROWS), BF16),
                pltpu.VMEM((YB * ch, YB * ch), BF16),
                pltpu.VMEM((2 * nyh * ROWS, batch * lanes), BF16),
                pltpu.VMEM((nyh * ROWS, batch * lanes), BF16),
                dma((chunks, pairs)), dma((chunks, pairs)),
                dma((4, chunks)), dma((4, chunks)), dma((xl,)), dma((chunks, xl)),
            ],
            compiler_params=pltpu.CompilerParams(
                collective_id=0, has_side_effects=True, vmem_limit_bytes=VMEM
            ),
        )(sample, target, weights, w_local, *tables)

        per = modes // pairs
        grad, grad_w = pl.pallas_call(
            make_last(fold, packed, chunks),
            grid=(pairs,),
            in_specs=[
                pl.BlockSpec((PAIR, ny, ch, nz), lambda i: (i, 0, 0, 0)),
                pl.BlockSpec((chunks, PAIR, nyh * ROWS, lanes), lambda i: (0, i, 0, 0)),
                whole(t["z_adj"]),
                pl.BlockSpec((per, 2 * pd, 2 * ch), lambda i: (i, 0, 0)),
                pl.BlockSpec((per, 2 * pd, 2 * ch), lambda i: (i, 0, 0)),
            ],
            out_specs=[
                pl.BlockSpec((PAIR, ny, ch, nz), lambda i: (i, 0, 0, 0)),
                pl.BlockSpec((per, ch, 2 * ch), lambda i: (i, 0, 0)),
            ],
            out_shape=[
                jax.ShapeDtypeStruct(sample.shape, BF16),
                jax.ShapeDtypeStruct((modes, ch, 2 * ch), F32),
            ],
            compiler_params=pltpu.CompilerParams(
                dimension_semantics=("arbitrary",), vmem_limit_bytes=VMEM
            ),
        )(spread, columns, t["z_adj"], ucat, gcat)
        return grad[None], grad_w.reshape(w_spec.shape)

    grid_spec = P("dp", "pencil", None, None, None)
    return jax.shard_map(
        body,
        mesh=mesh,
        in_specs=(grid_spec, grid_spec, grid_spec, P()),
        out_specs=(grid_spec, grid_spec),
        check_vma=False,
    )
```

```python
import math

import jax
import jax.numpy as jnp
import numpy as np
from jax import lax
from jax.experimental import pallas as pl
from jax.experimental.pallas import tpu as pltpu
from jax.sharding import PartitionSpec as P

BF16 = jnp.bfloat16
F32 = jnp.float32
ROWS = 16
PAIR = 2
YB = 4
BATCH = 8
LAST = 4
VMEM = 67043328
MESH = pl.DeviceIdType.MESH


def waves(length, count, signed, positions=None):
    index = np.arange(count)
    freq = np.where(index < count // 2, index, index - count) if signed else index
    place = np.arange(length if positions is None else positions)
    angle = 2.0 * math.pi * ((place[:, None] * freq[None, :]) % length) / length
    return np.cos(angle), np.sin(angle)


def const(array):
    return jnp.asarray(np.asarray(array, np.float32), BF16)


def make_tables(nx, ny, nz, fold, packed, mx, my, mz, pencils):
    cx, sx = waves(nx, mx, True)
    cy, sy = waves(ny, my, True, ny // fold)
    cz, sz = waves(nz, mz, False)
    eye_t = np.eye(fold * packed)
    plain = np.concatenate([cz, -sz], 1)
    turned = np.concatenate([-sz, -cz], 1)
    z_fwd = np.concatenate([np.kron(eye_t, plain), np.kron(eye_t, turned)], 1)
    weight = np.where(np.arange(mz) == 0, 1.0, 2.0) / (nx * ny * nz)
    z_inv = np.kron(eye_t, np.concatenate([cz * weight, -sz * weight], 1).T) * math.sqrt(0.5)
    z_adj = np.kron(eye_t, plain.T)
    half = np.eye(mz)
    zero = np.zeros((mz, mz))
    block = np.block([[zero, -half], [half, zero]])
    turn_t = np.kron(eye_t, block)
    turn = np.kron(np.eye(2), turn_t)
    lanes = fold * packed * 2 * mz
    r_fwd = np.zeros((fold, packed, fold, 2 * mz, packed, fold, 2 * mz))
    r_inv = np.zeros((packed, fold, 2 * mz, fold, packed, fold, 2 * mz))
    for b in range(fold):
        for h in range(fold):
            angle = 2.0 * math.pi * ((b * h) % fold) / fold
            c, s = np.cos(angle) * half, np.sin(angle) * half
            for g in range(packed):
                r_fwd[b, g, h, :, g, b, :] = np.block([[c, -s], [s, c]])
                r_inv[g, b, :, b, g, h, :] = np.block([[c, s], [-s, c]])
    r_fwd = r_fwd.reshape(fold * lanes, lanes)
    r_inv = r_inv.reshape(lanes, fold * lanes)
    r_fwd = np.concatenate([r_fwd, r_fwd @ turn_t], 1)
    r_inv = np.concatenate([r_inv, r_inv @ np.kron(np.eye(fold), turn_t)], 1)
    own = nx // pencils
    cx, sx = cx.reshape(pencils, own, mx), sx.reshape(pencils, own, mx)
    y_fwd = np.stack([cy.T, sy.T])
    y_inv = np.stack([cy, -sy])
    x_fwd = np.stack([cx.transpose(0, 2, 1), sx.transpose(0, 2, 1)], 1)
    x_inv = np.stack([cx, -sx], 1)
    scale = 0.5 * np.tile(np.concatenate([weight, weight]), fold * packed)[None]
    return dict(
        z_fwd=const(z_fwd), z_inv=const(z_inv), z_adj=const(z_adj), turn=const(turn),
        y_fwd=const(y_fwd), y_inv=const(y_inv), r_fwd=const(r_fwd), r_inv=const(r_inv),
        x_fwd=const(x_fwd), x_inv=const(x_inv),
        scale=jnp.asarray(np.asarray(scale, np.float32)),
    )


def mm(a, b):
    return jnp.dot(a, b, preferred_element_type=F32)


def twice_gelu_slope(q):
    bell = jnp.exp2((q * q) * (-1.0 / math.log(2.0)))
    return (1.0 + lax.erf(q)) + q * bell * (2.0 / math.sqrt(math.pi))


def expand(small):
    a, b = small.shape
    shift = ROWS.bit_length() - 1

    def iota(shape, axis):
        return lax.broadcasted_iota(jnp.int32, shape, axis)

    def same(left, right):
        return jnp.where(left == right, 1.0, 0.0).astype(BF16)

    tall, wide, full = (a * ROWS, a), (b, b * ROWS), (a * ROWS, b * ROWS)
    up = same(iota(tall, 0) >> shift, iota(tall, 1))
    out = same(iota(wide, 0), iota(wide, 1) >> shift)
    value = mm(mm(up, small).astype(BF16), out)
    return jnp.where((iota(full, 0) & (ROWS - 1)) == (iota(full, 1) & (ROWS - 1)), value, 0.0).astype(BF16)


def rows_of(index):
    return pl.ds(pl.multiple_of(index * ROWS, ROWS), ROWS)


def make_main(dims):
    pd, pp, jxl, jyl, mz, fold, packed, chunks = dims
    n = pd * pp
    nq = jyl // fold
    my = jyl * pp
    lanes = packed * fold * 2 * mz
    hm = fold * mz

    def kernel(
        field, cot, w, w_local, z_fwd, y_small, r_fwd, x_small, x_back, turn, r_inv, y_back, z_inv, scale,
        spread, columns, ucat, gcat,
        fbuf, cbuf, cols, sect, plain_in, turned_in, usend, vsend, bsend,
        urecv, vrecv, grecv, brecv, wbig, tbuf, obuf, xf, xi, y_fwd, y_inv, mixer, staged, cstage,
        fsem, csem, ssem, rsem, csend, crecv, relayed, osem, colsem,
    ):
        xl, ny, ch, nz = fbuf.shape
        nyh = ny // fold
        pairs = xl // PAIR
        batch = staged.shape[1] // lanes
        batches = xl // batch
        my_d, my_p = lax.axis_index("dp"), lax.axis_index("pencil")
        me = my_d * pp + my_p
        width = packed * ROWS

        barrier = pltpu.get_barrier_semaphore()

        def greet(i, carry):
            t = lax.rem(me + i, n)
            pl.semaphore_signal(
                barrier, inc=1, device_id=(lax.div(t, pp), lax.rem(t, pp)), device_id_type=MESH
            )
            return carry

        lax.fori_loop(1, n, greet, 0)

        def piece(ref, g, i):
            return ref.at[pl.ds(i * PAIR, PAIR), :, pl.ds(pl.multiple_of(g * width, width), width), :]

        def load(src, dst, sem, g, i):
            return pltpu.make_async_copy(piece(src, g, i), piece(dst, g, i), sem.at[g, i])

        def start_all(src, dst, sem):
            def one(j, carry):
                load(src, dst, sem, j // pairs, lax.rem(j, pairs)).start()
                return carry

            lax.fori_loop(0, chunks * pairs, one, 0)

        start_all(field, fbuf, fsem)
        start_all(cot, cbuf, csem)

        def fill(table, small):
            half = table.shape[1] // 2
            for part in range(2):
                table[:, part * half : (part + 1) * half] = expand(small[part])

        fill(y_fwd, y_small)
        fill(xf, x_small.at[my_p])

        def start_sends(source, recv, e, g):
            def one(i, carry):
                t = lax.rem(me + i, n)
                pltpu.make_async_remote_copy(
                    src_ref=source(t), dst_ref=recv.at[g, me],
                    send_sem=ssem.at[e, g], recv_sem=rsem.at[e, g],
                    device_id=(lax.div(t, pp), lax.rem(t, pp)), device_id_type=MESH,
                ).start()
                return carry

            lax.fori_loop(1, n, one, 0, unroll=8)
            pltpu.make_async_copy(source(me), recv.at[g, me], rsem.at[e, g]).start()

        def wait_recv(recv, e, g):
            pltpu.make_async_copy(recv.at[g], recv.at[g], rsem.at[e, g]).wait()

        def wait_sends(recv, e):
            def one(g, carry):
                sent = recv.at[g, pl.ds(0, n - 1)]
                pltpu.make_async_copy(sent, sent, ssem.at[e, g]).wait()
                return carry

            lax.fori_loop(0, chunks, one, 0)

        half = pp // 2
        side = lax.div(my_p, half)
        reach = half + 1
        lowest = side * (half - 1)

        def start_cast(source, recv, e, g):
            place = my_p * pd + my_d
            own = my_d * reach + my_p - lowest

            def one(i, carry):
                t = lax.rem(own + i, pd * reach)
                s = lax.div(t, reach)
                pltpu.make_async_remote_copy(
                    src_ref=source.at[g, s], dst_ref=recv.at[g, place],
                    send_sem=csend.at[e, g], recv_sem=crecv.at[e, side, g],
                    device_id=(s, lowest + lax.rem(t, reach)), device_id_type=MESH,
                ).start()
                return carry

            lax.fori_loop(1, pd * reach, one, 0, unroll=8)
            pltpu.make_async_copy(source.at[g, my_d], recv.at[g, place], crecv.at[e, side, g]).start()

        def part_of(recv, g, which):
            return recv.at[g, pl.ds(which * half * pd, half * pd)]

        def wait_part(recv, e, g, which):
            part = part_of(recv, g, which)
            pltpu.make_async_copy(part, part, crecv.at[e, which, g]).wait()

        def pass_on(recv, e, g, which, r):
            part = part_of(recv, g, which)
            target = half + 1 + r if which == 0 else r
            return pltpu.make_async_remote_copy(
                src_ref=part, dst_ref=part,
                send_sem=relayed.at[e, g, r], recv_sem=crecv.at[e, which, g],
                device_id=(my_d, target), device_id_type=MESH,
            )

        def relay(recv, e, g):
            for which in range(2):

                @pl.when(my_p == half - which)
                def _():
                    wait_part(recv, e, g, which)
                    for r in range(half - 1):
                        pass_on(recv, e, g, which, r).start()

        def wait_cast(recv, e, g):
            for which in range(2):

                @pl.when(my_p != half - which)
                def _():
                    wait_part(recv, e, g, which)

        def end_cast(recv, e):
            def one(g, carry):
                sent = recv.at[g, pl.ds(0, pd * reach - 1)]
                pltpu.make_async_copy(sent, sent, csend.at[e, g]).wait()
                for which in range(2):

                    @pl.when(my_p == half - which)
                    def _():
                        part = part_of(recv, g, which)
                        for r in range(half - 1):
                            pltpu.make_async_copy(part, part, relayed.at[e, g, r]).wait()

                return carry

            lax.fori_loop(0, chunks, one, 0)

        def forward_z(wide, e):
            spectral = mm(wide, z_fwd[...]).astype(BF16)
            rows = nyh * ROWS
            staged[:rows, e * lanes : (e + 1) * lanes] = spectral[:, :lanes]
            staged[rows:, e * lanes : (e + 1) * lanes] = spectral[:, lanes:]

        def forward_y(x0):
            for k in range(0, batch, PAIR):
                out = mm(y_fwd[...], staged[:, k * lanes : (k + PAIR) * lanes]).astype(BF16)
                for e in range(PAIR):
                    sect[x0 + k + e] = out[:, e * lanes : (e + 1) * lanes]

        def forward_x(send, g):
            tiles = my // fold
            for q0 in range(0, tiles, 2):
                group = range(q0, min(q0 + 2, tiles))
                plain, turned = [], []
                for q in group:
                    rows = jnp.concatenate(
                        [
                            sect[:, (q * fold + b) * ROWS : (q * fold + b + 1) * ROWS, :].reshape(xl * ROWS, lanes)
                            for b in range(fold)
                        ],
                        1,
                    )
                    both = mm(rows, r_fwd[...]).astype(BF16)
                    plain.append(both[:, :lanes])
                    turned.append(both[:, lanes:])
                stacked = jnp.concatenate([jnp.concatenate(plain, 1), jnp.concatenate(turned, 1)], 0)
                got = mm(xf[...], stacked).astype(BF16)
                for e, q in enumerate(group):
                    for d in range(pd):
                        send[g, d * pp + q // nq, q % nq] = got[
                            d * jxl * ROWS : (d + 1) * jxl * ROWS, e * lanes : (e + 1) * lanes
                        ]

        def inverse_x(recv, g):
            tiles = my // fold
            for q0 in range(0, tiles, 2):
                group = range(q0, min(q0 + 2, tiles))
                rows = jnp.concatenate(
                    [
                        jnp.concatenate([recv[g, (q // nq) * pd + d, q % nq] for d in range(pd)], 0)
                        for q in group
                    ],
                    1,
                )
                size = rows.shape[1]
                turned = mm(rows, turn[:size, :size]).astype(BF16)
                got = mm(xi[...], jnp.concatenate([rows, turned], 0)).astype(BF16)
                for e, q in enumerate(group):
                    wide = mm(got[:, e * lanes : (e + 1) * lanes], r_inv[...]).astype(BF16)
                    for b in range(fold):
                        j = q * fold + b
                        at = slice(j * ROWS, (j + 1) * ROWS)
                        plain_in[:, at, :] = wide[:, b * lanes : (b + 1) * lanes].reshape(xl, ROWS, lanes)
                        turned_in[:, at, :] = wide[
                            :, (fold + b) * lanes : (fold + b + 1) * lanes
                        ].reshape(xl, ROWS, lanes)

        def inverse_y(x0):
            stacked = jnp.concatenate(
                [
                    jnp.concatenate([plain_in[x0 + e] for e in range(PAIR)], 1),
                    jnp.concatenate([turned_in[x0 + e] for e in range(PAIR)], 1),
                ],
                0,
            )
            return mm(y_inv[...], stacked).astype(BF16)

        def places(g):
            for gi in range(packed):
                for h in range(fold):
                    yield pl.ds(h * nyh, nyh), rows_of(g * packed + gi), (gi * fold + h) * nz

        def mix(matrix, factor):
            tiled = jnp.concatenate([matrix] * YB, 1)
            owner = lax.broadcasted_iota(jnp.int32, (1, YB * ch), 1) // ch
            for b in range(YB):
                mixer[b * ch : (b + 1) * ch, :] = jnp.where(owner == b, tiled, 0.0).astype(BF16)

            steps = math.gcd(ny // YB, 16)
            per = ny // YB // steps

            def one(j, carry):
                x0 = (j // per) * PAIR
                y0 = lax.rem(j, per) * (YB * steps)
                for u in range(steps):
                    ys = pl.ds(y0 + u * YB, YB)
                    wide = jnp.concatenate([fbuf[x0 + e, ys].reshape(YB * ch, nz) for e in range(PAIR)], 1)
                    mixed = (mm(mixer[...], wide) * factor).astype(BF16)
                    for e in range(PAIR):
                        fbuf[x0 + e, ys] = mixed[:, e * nz : (e + 1) * nz].reshape(YB, ch, nz)
                return carry

            lax.fori_loop(0, pairs * per, one, 0)

        def load_modes(recv, scaled):
            for jx in range(jxl):
                for ql in range(nq):
                    blocks = []
                    for s in range(pd):
                        for c in range(chunks):
                            at = slice(jx * ROWS, (jx + 1) * ROWS)
                            total = recv[c, s * pp, ql, at, :].astype(F32)
                            for q in range(1, pp):
                                total = total + recv[c, s * pp + q, ql, at, :].astype(F32)
                            blocks.append(total)
                    value = jnp.concatenate(blocks, 0)
                    if scaled:
                        value = value * scale[...]
                    flat = value.T
                    for s in range(pd):
                        for b in range(fold):
                            parts = []
                            for ri in range(2):
                                for c in range(chunks):
                                    for gi in range(packed):
                                        top = ((gi * fold + b) * 2 + ri) * mz
                                        left = (s * chunks + c) * ROWS
                                        if packed == 1 and c == 0:
                                            parts.append(flat[top : top + mz, left : left + ch])
                                        elif packed > 1:
                                            parts.append(flat[top : top + mz, left : left + ROWS])
                            low = s * hm + b * mz
                            tbuf[jx * nq + ql, low : low + mz, :] = jnp.concatenate(parts, 1)

        def store_modes(send):
            for jx in range(jxl):
                for ql in range(nq):
                    columns_of = []
                    for s in range(pd):
                        own = obuf[jx * nq + ql, s * hm : (s + 1) * hm, :]
                        if packed == 1:
                            columns_of.append(
                                jnp.concatenate(
                                    [
                                        own[b * mz : (b + 1) * mz, ri * ch : (ri + 1) * ch]
                                        for b in range(fold)
                                        for ri in range(2)
                                    ],
                                    0,
                                )
                            )
                        else:
                            for c in range(chunks):
                                columns_of.append(
                                    jnp.concatenate(
                                        [
                                            own[
                                                b * mz : (b + 1) * mz,
                                                ri * ch + (c * packed + gi) * ROWS : ri * ch + (c * packed + gi + 1) * ROWS,
                                            ]
                                            for gi in range(packed)
                                            for b in range(fold)
                                            for ri in range(2)
                                        ],
                                        0,
                                    )
                                )
                    back = jnp.concatenate(columns_of, 1).T.astype(BF16)
                    for s in range(pd):
                        for c in range(chunks):
                            low = (s * chunks + c) * ROWS
                            send[c, s, ql, jx * ROWS : (jx + 1) * ROWS, :] = back[low : low + ROWS, :]

        def each_mode(apply):
            def one(jq, carry):
                for r in range(hm):
                    own = tbuf[jq, pl.ds(r, pd, stride=hm), :]
                    obuf[jq, pl.ds(r, pd, stride=hm), :] = apply(jq * hm + r, own)
                return carry

            lax.fori_loop(0, jxl * nq, one, 0)

        def first(g, carry):
            def one(i, inner):
                x0 = i * batch
                for k in range(batch // PAIR):
                    load(field, fbuf, fsem, g, i * (batch // PAIR) + k).wait()
                for e in range(batch):
                    forward_z(
                        jnp.concatenate(
                            [fbuf[x0 + e, ys, cs, :].reshape(nyh * ROWS, nz) for ys, cs, _ in places(g)], 1
                        ),
                        e,
                    )
                forward_y(x0)
                return inner

            lax.fori_loop(0, batches, one, 0)
            forward_x(usend, g)

            @pl.when(g == 0)
            def _():
                pl.semaphore_wait(barrier, n - 1)

            start_sends(lambda t: usend.at[g, t], urecv, 0, g)
            return carry

        lax.fori_loop(0, chunks, first, 0)

        sign = jnp.where(lax.broadcasted_iota(jnp.int32, (1, 2 * ch), 1) < ch, -1.0, 1.0).astype(F32)

        def prepare(m, carry):
            own = w[m].astype(F32)
            wbig[m, :ch, :] = w[m]
            wbig[m, ch:, :] = (pltpu.roll(own, ch, 1) * sign).astype(BF16)
            return carry

        lax.fori_loop(0, w.shape[0], prepare, 0, unroll=4)
        fill(y_inv, y_back)
        fill(xi, x_back.at[my_p])
        mix(w_local[...].astype(F32).T, math.sqrt(0.5))

        def waits(recv, e):
            def one(g, carry):
                wait_recv(recv, e, g)
                return carry

            lax.fori_loop(0, chunks, one, 0)

        waits(urecv, 0)
        load_modes(urecv, False)

        def apply_one(m, own):
            ucat[m] = jnp.concatenate([own, pltpu.roll(own, ch, 1)], 0).astype(BF16)
            return mm(own.astype(BF16), wbig[m])

        each_mode(apply_one)
        store_modes(vsend)

        def send_v(g, carry):
            start_cast(vsend, vrecv, 0, g)
            return carry

        lax.fori_loop(0, chunks, send_v, 0)
        wait_sends(urecv, 0)

        def middle(g, carry):
            @pl.when(g == 0)
            def _():
                relay(vrecv, 0, g)

            wait_cast(vrecv, 0, g)
            inverse_x(vrecv, g)

            @pl.when(g < chunks - 1)
            def _():
                relay(vrecv, 0, g + 1)


            def one(i, inner):
                x0 = i * batch
                for k in range(batch // PAIR):
                    load(cot, cbuf, csem, g, i * (batch // PAIR) + k).wait()
                for k in range(0, batch, PAIR):
                    cstage[:, k * lanes : (k + PAIR) * lanes] = inverse_y(x0 + k)
                for e in range(batch):
                    grid = mm(cstage[:, e * lanes : (e + 1) * lanes], z_inv[...])
                    pieces = []
                    for ys, cs, left in places(g):
                        q = grid[:, left : left + nz].reshape(nyh, ROWS, nz) + fbuf[x0 + e, ys, cs, :].astype(F32)
                        slope = (cbuf[x0 + e, ys, cs, :].astype(F32) * twice_gelu_slope(q)).astype(BF16)
                        fbuf[x0 + e, ys, cs, :] = slope
                        pieces.append(slope.reshape(nyh * ROWS, nz))
                    forward_z(jnp.concatenate(pieces, 1), e)
                forward_y(x0)
                return inner

            lax.fori_loop(0, batches, one, 0)
            forward_x(usend, g)
            start_sends(lambda t: usend.at[g, t], grecv, 1, g)
            return carry

        lax.fori_loop(0, chunks, middle, 0)

        mix(w_local[...].astype(F32) * 0.5, 1.0)

        def spread_out(x):
            return pltpu.make_async_copy(fbuf.at[x], spread.at[x], osem.at[x])

        def put(x, carry):
            spread_out(x).start()
            return carry

        lax.fori_loop(0, xl, put, 0)

        waits(grecv, 1)
        load_modes(grecv, True)

        def adjoint_one(m, own):
            own = own.astype(BF16).astype(F32)
            gcat[m] = jnp.concatenate([own, pltpu.roll(own, ch, 1) * -sign], 0).astype(BF16)
            return lax.dot_general(
                own.astype(BF16), wbig[m], (((1,), (1,)), ((), ())), preferred_element_type=F32
            )

        each_mode(adjoint_one)
        store_modes(bsend)

        def send_b(g, carry):
            start_cast(bsend, brecv, 1, g)
            return carry

        lax.fori_loop(0, chunks, send_b, 0)

        def cols_out(g, x):
            return pltpu.make_async_copy(cols.at[g, x], columns.at[g, x], colsem.at[g, x])

        def last(g, carry):
            relay(brecv, 1, g)
            wait_cast(brecv, 1, g)
            inverse_x(brecv, g)

            def one(i, inner):
                for k in range(0, batch, PAIR):
                    x0 = i * batch + k
                    col = inverse_y(x0)
                    for e in range(PAIR):
                        cols[g, x0 + e] = col[:, e * lanes : (e + 1) * lanes]
                return inner

            lax.fori_loop(0, batches, one, 0)

            def out(x, inner):
                cols_out(g, x).start()
                return inner

            lax.fori_loop(0, xl, out, 0)
            return carry

        lax.fori_loop(0, chunks, last, 0)
        end_cast(vrecv, 0)
        wait_sends(grecv, 1)
        end_cast(brecv, 1)

        def finish(x, carry):
            spread_out(x).wait()
            for g in range(chunks):
                cols_out(g, x).wait()
            return carry

        lax.fori_loop(0, xl, finish, 0)

    return kernel


def make_last(fold, packed, chunks):
    def kernel(spread, columns, z_adj, ucat, gcat, grad, grad_w):
        xs, ny, ch, nz = spread.shape
        nyh = ny // fold
        for x in range(xs):
            for g in range(chunks):
                grid = mm(columns[g, x], z_adj[...])
                for gi in range(packed):
                    for h in range(fold):
                        left = (gi * fold + h) * nz
                        ys = slice(h * nyh, (h + 1) * nyh)
                        cs = slice((g * packed + gi) * ROWS, (g * packed + gi + 1) * ROWS)
                        value = grid[:, left : left + nz].reshape(nyh, ROWS, nz)
                        grad[x, ys, cs, :] = (value + spread[x, ys, cs, :].astype(F32)).astype(BF16)
        for m in range(grad_w.shape[0]):
            grad_w[m] = lax.dot_general(
                ucat[m], gcat[m], (((0,), (0,)), ((), ())), preferred_element_type=F32
            )[:ch]

    return kernel


def whole(array):
    return pl.BlockSpec(array.shape, lambda i, n=len(array.shape): (0,) * n)


def solution(mesh):
    pd, pp = mesh.shape["dp"], mesh.shape["pencil"]

    def body(field, cotangent, w_spec, w_local):
        sample, target = field[0], cotangent[0]
        xl, ny, ch, nz = sample.shape
        jxl, jyl, mz = w_spec.shape[:3]
        mx, my = jxl * pd, jyl * pp
        groups = ch // ROWS
        fold = math.gcd(jyl, groups)
        packed = groups // fold
        chunks = groups // packed
        lanes = groups * 2 * mz
        nq = jyl // fold
        n = pd * pp
        modes = jxl * jyl * mz
        pairs = xl // PAIR
        nyh = ny // fold
        t = make_tables(xl * pp, ny, nz, fold, packed, mx, my, mz, pp)
        weights = w_spec.reshape(modes, ch, 2 * ch)
        hbm = pl.BlockSpec(memory_space=pl.ANY)
        vmem = pl.BlockSpec(memory_space=pltpu.VMEM)
        names = ("z_fwd", "y_fwd", "r_fwd", "x_fwd", "x_inv", "turn", "r_inv", "y_inv", "z_inv", "scale")
        tables = [t[name] for name in names]
        table_specs = [vmem] * len(names)
        batch = math.gcd(xl, BATCH)
        block = (nq, jxl * ROWS, lanes)
        part = pltpu.VMEM((chunks, n) + block, BF16)
        mode_part = pltpu.VMEM((chunks, pd) + block, BF16)
        section = pltpu.VMEM((xl, my * ROWS, lanes), BF16)
        grid_buf = pltpu.VMEM(sample.shape, BF16)
        by_mode = pltpu.VMEM((jxl * nq, pd * fold * mz, 2 * ch), F32)
        dma = pltpu.SemaphoreType.DMA
        dims = (pd, pp, jxl, jyl, mz, fold, packed, chunks)
        cat = jax.ShapeDtypeStruct((modes, 2 * pd, 2 * ch), BF16)
        spread, columns, ucat, gcat = pl.pallas_call(
            make_main(dims),
            in_specs=[hbm, hbm, vmem, vmem] + table_specs,
            out_specs=[hbm, hbm, vmem, vmem],
            out_shape=[
                jax.ShapeDtypeStruct(sample.shape, BF16),
                jax.ShapeDtypeStruct((chunks, xl, nyh * ROWS, lanes), BF16),
                cat,
                cat,
            ],
            scratch_shapes=[
                grid_buf, grid_buf,
                pltpu.VMEM((chunks, xl, nyh * ROWS, lanes), BF16),
                section, section, section,
                part, mode_part, mode_part,
                part, part, part, part,
                pltpu.VMEM((modes, 2 * ch, 2 * ch), BF16),
                by_mode, by_mode,
                pltpu.VMEM((mx * ROWS, 2 * xl * ROWS), BF16),
                pltpu.VMEM((xl * ROWS, 2 * mx * ROWS), BF16),
                pltpu.VMEM((my * ROWS, 2 * nyh * ROWS), BF16),
                pltpu.VMEM((nyh * ROWS, 2 * my * ROWS), BF16),
                pltpu.VMEM((YB * ch, YB * ch), BF16),
                pltpu.VMEM((2 * nyh * ROWS, batch * lanes), BF16),
                pltpu.VMEM((nyh * ROWS, batch * lanes), BF16),
                dma((chunks, pairs)), dma((chunks, pairs)),
                dma((2, chunks)), dma((2, chunks)),
                dma((2, chunks)), dma((2, 2, chunks)), dma((2, chunks, max(pp // 2 - 1, 1))), dma((xl,)), dma((chunks, xl)),
            ],
            compiler_params=pltpu.CompilerParams(
                collective_id=0, has_side_effects=True, vmem_limit_bytes=VMEM
            ),
        )(sample, target, weights, w_local, *tables)

        rows = math.gcd(xl, LAST)
        steps = xl // rows
        per = modes // steps
        grad, grad_w = pl.pallas_call(
            make_last(fold, packed, chunks),
            grid=(steps,),
            in_specs=[
                pl.BlockSpec((rows, ny, ch, nz), lambda i: (i, 0, 0, 0)),
                pl.BlockSpec((chunks, rows, nyh * ROWS, lanes), lambda i: (0, i, 0, 0)),
                whole(t["z_adj"]),
                pl.BlockSpec((per, 2 * pd, 2 * ch), lambda i: (i, 0, 0)),
                pl.BlockSpec((per, 2 * pd, 2 * ch), lambda i: (i, 0, 0)),
            ],
            out_specs=[
                pl.BlockSpec((rows, ny, ch, nz), lambda i: (i, 0, 0, 0)),
                pl.BlockSpec((per, ch, 2 * ch), lambda i: (i, 0, 0)),
            ],
            out_shape=[
                jax.ShapeDtypeStruct(sample.shape, BF16),
                jax.ShapeDtypeStruct((modes, ch, 2 * ch), F32),
            ],
            compiler_params=pltpu.CompilerParams(
                dimension_semantics=("arbitrary",), vmem_limit_bytes=VMEM
            ),
        )(spread, columns, t["z_adj"], ucat, gcat)
        return grad[None], grad_w.reshape(w_spec.shape)

    grid_spec = P("dp", "pencil", None, None, None)
    return jax.shard_map(
        body,
        mesh=mesh,
        in_specs=(grid_spec, grid_spec, grid_spec, P()),
        out_specs=(grid_spec, grid_spec),
        check_vma=False,
    )
```

```python
import math

import jax
import jax.numpy as jnp
import numpy as np
from jax import lax
from jax.experimental import pallas as pl
from jax.experimental.pallas import tpu as pltpu
from jax.sharding import PartitionSpec as P

BF16 = jnp.bfloat16
F32 = jnp.float32
ROWS = 16
PAIR = 2
YB = 4
BATCH = 8
LAST = 4
VMEM = 67043328
MESH = pl.DeviceIdType.MESH


def waves(length, count, signed, positions=None):
    index = np.arange(count)
    freq = np.where(index < count // 2, index, index - count) if signed else index
    place = np.arange(length if positions is None else positions)
    angle = 2.0 * math.pi * ((place[:, None] * freq[None, :]) % length) / length
    return np.cos(angle), np.sin(angle)


def const(array):
    return jnp.asarray(np.asarray(array, np.float32), BF16)


def make_tables(nx, ny, nz, fold, packed, mx, my, mz, pencils):
    cx, sx = waves(nx, mx, True)
    cy, sy = waves(ny, my, True, ny // fold)
    cz, sz = waves(nz, mz, False)
    eye_t = np.eye(fold * packed)
    plain = np.concatenate([cz, -sz], 1)
    turned = np.concatenate([-sz, -cz], 1)
    z_fwd = np.concatenate([np.kron(eye_t, plain), np.kron(eye_t, turned)], 1)
    weight = np.where(np.arange(mz) == 0, 1.0, 2.0) / (nx * ny * nz)
    z_inv = np.kron(eye_t, np.concatenate([cz * weight, -sz * weight], 1).T) * math.sqrt(0.5)
    z_adj = np.kron(eye_t, plain.T)
    half = np.eye(mz)
    zero = np.zeros((mz, mz))
    block = np.block([[zero, -half], [half, zero]])
    turn_t = np.kron(eye_t, block)
    turn = np.kron(np.eye(2), turn_t)
    lanes = fold * packed * 2 * mz
    r_fwd = np.zeros((fold, packed, fold, 2 * mz, packed, fold, 2 * mz))
    r_inv = np.zeros((packed, fold, 2 * mz, fold, packed, fold, 2 * mz))
    for b in range(fold):
        for h in range(fold):
            angle = 2.0 * math.pi * ((b * h) % fold) / fold
            c, s = np.cos(angle) * half, np.sin(angle) * half
            for g in range(packed):
                r_fwd[b, g, h, :, g, b, :] = np.block([[c, -s], [s, c]])
                r_inv[g, b, :, b, g, h, :] = np.block([[c, s], [-s, c]])
    r_fwd = r_fwd.reshape(fold * lanes, lanes)
    r_inv = r_inv.reshape(lanes, fold * lanes)
    r_fwd = np.concatenate([r_fwd, r_fwd @ turn_t], 1)
    r_inv = np.concatenate([r_inv, r_inv @ np.kron(np.eye(fold), turn_t)], 1)
    own = nx // pencils
    cx, sx = cx.reshape(pencils, own, mx), sx.reshape(pencils, own, mx)
    y_fwd = np.stack([cy.T, sy.T])
    y_inv = np.stack([cy, -sy])
    x_fwd = np.stack([cx.transpose(0, 2, 1), sx.transpose(0, 2, 1)], 1)
    x_inv = np.stack([cx, -sx], 1)
    scale = 0.5 * np.tile(np.concatenate([weight, weight]), fold * packed)[None]
    return dict(
        z_fwd=const(z_fwd), z_inv=const(z_inv), z_adj=const(z_adj), turn=const(turn),
        y_fwd=const(y_fwd), y_inv=const(y_inv), r_fwd=const(r_fwd), r_inv=const(r_inv),
        x_fwd=const(x_fwd), x_inv=const(x_inv),
        scale=jnp.asarray(np.asarray(scale, np.float32)),
    )


def mm(a, b):
    return jnp.dot(a, b, preferred_element_type=F32)


def twice_gelu_slope(q):
    bell = jnp.exp2((q * q) * (-1.0 / math.log(2.0)))
    return (1.0 + lax.erf(q)) + q * bell * (2.0 / math.sqrt(math.pi))


def expand(small):
    a, b = small.shape
    shift = ROWS.bit_length() - 1

    def iota(shape, axis):
        return lax.broadcasted_iota(jnp.int32, shape, axis)

    def same(left, right):
        return jnp.where(left == right, 1.0, 0.0).astype(BF16)

    tall, wide, full = (a * ROWS, a), (b, b * ROWS), (a * ROWS, b * ROWS)
    up = same(iota(tall, 0) >> shift, iota(tall, 1))
    out = same(iota(wide, 0), iota(wide, 1) >> shift)
    value = mm(mm(up, small).astype(BF16), out)
    return jnp.where((iota(full, 0) & (ROWS - 1)) == (iota(full, 1) & (ROWS - 1)), value, 0.0).astype(BF16)


def rows_of(index):
    return pl.ds(pl.multiple_of(index * ROWS, ROWS), ROWS)


def make_main(dims):
    pd, pp, jxl, jyl, mz, fold, packed, chunks = dims
    n = pd * pp
    nq = jyl // fold
    my = jyl * pp
    lanes = packed * fold * 2 * mz
    hm = fold * mz

    def kernel(
        field, cot, w, w_local, z_fwd, y_small, r_fwd, x_small, x_back, turn, r_inv, y_back, z_inv, scale,
        spread, columns, ucat, gcat,
        fbuf, cbuf, cols, sect, plain_in, turned_in, usend, vsend, bsend,
        urecv, vrecv, grecv, brecv, wbig, tbuf, obuf, xf, xi, y_fwd, y_inv, mixer, staged, cstage,
        fsem, csem, ssem, rsem, csend, crecv, relayed, osem, colsem,
    ):
        xl, ny, ch, nz = fbuf.shape
        nyh = ny // fold
        pairs = xl // PAIR
        batch = staged.shape[1] // lanes
        batches = xl // batch
        my_d, my_p = lax.axis_index("dp"), lax.axis_index("pencil")
        me = my_d * pp + my_p
        width = packed * ROWS

        barrier = pltpu.get_barrier_semaphore()

        def greet(i, carry):
            t = lax.rem(me + i, n)
            pl.semaphore_signal(
                barrier, inc=1, device_id=(lax.div(t, pp), lax.rem(t, pp)), device_id_type=MESH
            )
            return carry

        lax.fori_loop(1, n, greet, 0)

        def piece(ref, g, i):
            return ref.at[pl.ds(i * PAIR, PAIR), :, pl.ds(pl.multiple_of(g * width, width), width), :]

        def load(src, dst, sem, g, i):
            return pltpu.make_async_copy(piece(src, g, i), piece(dst, g, i), sem.at[g, i])

        def start_all(src, dst, sem):
            def one(j, carry):
                load(src, dst, sem, j // pairs, lax.rem(j, pairs)).start()
                return carry

            lax.fori_loop(0, chunks * pairs, one, 0)

        start_all(field, fbuf, fsem)
        start_all(cot, cbuf, csem)

        def fill(table, small):
            half = table.shape[1] // 2
            for part in range(2):
                table[:, part * half : (part + 1) * half] = expand(small[part])

        fill(y_fwd, y_small)
        fill(xf, x_small.at[my_p])

        def start_sends(source, recv, e, g):
            def one(i, carry):
                t = lax.rem(me + i, n)
                pltpu.make_async_remote_copy(
                    src_ref=source(t), dst_ref=recv.at[g, me],
                    send_sem=ssem.at[e, g], recv_sem=rsem.at[e, g],
                    device_id=(lax.div(t, pp), lax.rem(t, pp)), device_id_type=MESH,
                ).start()
                return carry

            lax.fori_loop(1, n, one, 0, unroll=8)
            pltpu.make_async_copy(source(me), recv.at[g, me], rsem.at[e, g]).start()

        def wait_recv(recv, e, g):
            pltpu.make_async_copy(recv.at[g], recv.at[g], rsem.at[e, g]).wait()

        def wait_sends(recv, e):
            def one(g, carry):
                sent = recv.at[g, pl.ds(0, n - 1)]
                pltpu.make_async_copy(sent, sent, ssem.at[e, g]).wait()
                return carry

            lax.fori_loop(0, chunks, one, 0)

        half = pp // 2
        side = lax.div(my_p, half)
        reach = half + 1

        def start_cast(source, recv, e, g):
            place = my_p * pd + my_d

            def send(s, q):
                pltpu.make_async_remote_copy(
                    src_ref=source.at[g, s], dst_ref=recv.at[g, place],
                    send_sem=csend.at[e, g], recv_sem=crecv.at[e, side, g],
                    device_id=(s, q), device_id_type=MESH,
                ).start()

            for step in range(reach):
                q = half - side + step * (2 * side - 1)

                def one(i, carry):
                    send(lax.rem(my_d + i, pd), q)
                    return carry

                lax.fori_loop(1, pd, one, 0, unroll=7)

                @pl.when(q != my_p)
                def _():
                    send(my_d, q)

            pltpu.make_async_copy(source.at[g, my_d], recv.at[g, place], crecv.at[e, side, g]).start()

        def part_of(recv, g, which):
            return recv.at[g, pl.ds(which * half * pd, half * pd)]

        def wait_part(recv, e, g, which):
            part = part_of(recv, g, which)
            pltpu.make_async_copy(part, part, crecv.at[e, which, g]).wait()

        def pass_on(recv, e, g, which, r):
            part = part_of(recv, g, which)
            target = half + 1 + r if which == 0 else r
            return pltpu.make_async_remote_copy(
                src_ref=part, dst_ref=part,
                send_sem=relayed.at[e, g, r], recv_sem=crecv.at[e, which, g],
                device_id=(my_d, target), device_id_type=MESH,
            )

        def relay(recv, e, g):
            for which in range(2):

                @pl.when(my_p == half - which)
                def _():
                    wait_part(recv, e, g, which)
                    for r in range(half - 1):
                        pass_on(recv, e, g, which, r).start()

        def wait_cast(recv, e, g):
            for which in range(2):

                @pl.when(my_p != half - which)
                def _():
                    wait_part(recv, e, g, which)

        def end_cast(recv, e):
            def one(g, carry):
                sent = recv.at[g, pl.ds(0, pd * reach - 1)]
                pltpu.make_async_copy(sent, sent, csend.at[e, g]).wait()
                for which in range(2):

                    @pl.when(my_p == half - which)
                    def _():
                        part = part_of(recv, g, which)
                        for r in range(half - 1):
                            pltpu.make_async_copy(part, part, relayed.at[e, g, r]).wait()

                return carry

            lax.fori_loop(0, chunks, one, 0)

        def forward_z(wide, e):
            spectral = mm(wide, z_fwd[...]).astype(BF16)
            rows = nyh * ROWS
            staged[:rows, e * lanes : (e + 1) * lanes] = spectral[:, :lanes]
            staged[rows:, e * lanes : (e + 1) * lanes] = spectral[:, lanes:]

        def forward_y(x0):
            for k in range(0, batch, PAIR):
                out = mm(y_fwd[...], staged[:, k * lanes : (k + PAIR) * lanes]).astype(BF16)
                for e in range(PAIR):
                    sect[x0 + k + e] = out[:, e * lanes : (e + 1) * lanes]

        def forward_x(send, g):
            tiles = my // fold
            for q0 in range(0, tiles, 2):
                group = range(q0, min(q0 + 2, tiles))
                plain, turned = [], []
                for q in group:
                    rows = jnp.concatenate(
                        [
                            sect[:, (q * fold + b) * ROWS : (q * fold + b + 1) * ROWS, :].reshape(xl * ROWS, lanes)
                            for b in range(fold)
                        ],
                        1,
                    )
                    both = mm(rows, r_fwd[...]).astype(BF16)
                    plain.append(both[:, :lanes])
                    turned.append(both[:, lanes:])
                stacked = jnp.concatenate([jnp.concatenate(plain, 1), jnp.concatenate(turned, 1)], 0)
                got = mm(xf[...], stacked).astype(BF16)
                for e, q in enumerate(group):
                    for d in range(pd):
                        send[g, d * pp + q // nq, q % nq] = got[
                            d * jxl * ROWS : (d + 1) * jxl * ROWS, e * lanes : (e + 1) * lanes
                        ]

        def inverse_x(recv, g):
            tiles = my // fold
            for q0 in range(0, tiles, 2):
                group = range(q0, min(q0 + 2, tiles))
                rows = jnp.concatenate(
                    [
                        jnp.concatenate([recv[g, (q // nq) * pd + d, q % nq] for d in range(pd)], 0)
                        for q in group
                    ],
                    1,
                )
                size = rows.shape[1]
                turned = mm(rows, turn[:size, :size]).astype(BF16)
                got = mm(xi[...], jnp.concatenate([rows, turned], 0)).astype(BF16)
                for e, q in enumerate(group):
                    wide = mm(got[:, e * lanes : (e + 1) * lanes], r_inv[...]).astype(BF16)
                    for b in range(fold):
                        j = q * fold + b
                        at = slice(j * ROWS, (j + 1) * ROWS)
                        plain_in[:, at, :] = wide[:, b * lanes : (b + 1) * lanes].reshape(xl, ROWS, lanes)
                        turned_in[:, at, :] = wide[
                            :, (fold + b) * lanes : (fold + b + 1) * lanes
                        ].reshape(xl, ROWS, lanes)

        def inverse_y(x0):
            stacked = jnp.concatenate(
                [
                    jnp.concatenate([plain_in[x0 + e] for e in range(PAIR)], 1),
                    jnp.concatenate([turned_in[x0 + e] for e in range(PAIR)], 1),
                ],
                0,
            )
            return mm(y_inv[...], stacked).astype(BF16)

        def places(g):
            for gi in range(packed):
                for h in range(fold):
                    yield pl.ds(h * nyh, nyh), rows_of(g * packed + gi), (gi * fold + h) * nz

        def mix(matrix, factor):
            tiled = jnp.concatenate([matrix] * YB, 1)
            owner = lax.broadcasted_iota(jnp.int32, (1, YB * ch), 1) // ch
            for b in range(YB):
                mixer[b * ch : (b + 1) * ch, :] = jnp.where(owner == b, tiled, 0.0).astype(BF16)

            steps = math.gcd(ny // YB, 16)
            per = ny // YB // steps

            def one(j, carry):
                x0 = (j // per) * PAIR
                y0 = lax.rem(j, per) * (YB * steps)
                for u in range(steps):
                    ys = pl.ds(y0 + u * YB, YB)
                    wide = jnp.concatenate([fbuf[x0 + e, ys].reshape(YB * ch, nz) for e in range(PAIR)], 1)
                    mixed = (mm(mixer[...], wide) * factor).astype(BF16)
                    for e in range(PAIR):
                        fbuf[x0 + e, ys] = mixed[:, e * nz : (e + 1) * nz].reshape(YB, ch, nz)
                return carry

            lax.fori_loop(0, pairs * per, one, 0)

        def load_modes(recv, scaled):
            for jx in range(jxl):
                for ql in range(nq):
                    blocks = []
                    for s in range(pd):
                        for c in range(chunks):
                            at = slice(jx * ROWS, (jx + 1) * ROWS)
                            total = recv[c, s * pp, ql, at, :].astype(F32)
                            for q in range(1, pp):
                                total = total + recv[c, s * pp + q, ql, at, :].astype(F32)
                            blocks.append(total)
                    value = jnp.concatenate(blocks, 0)
                    if scaled:
                        value = value * scale[...]
                    flat = value.T
                    for s in range(pd):
                        for b in range(fold):
                            parts = []
                            for ri in range(2):
                                for c in range(chunks):
                                    for gi in range(packed):
                                        top = ((gi * fold + b) * 2 + ri) * mz
                                        left = (s * chunks + c) * ROWS
                                        if packed == 1 and c == 0:
                                            parts.append(flat[top : top + mz, left : left + ch])
                                        elif packed > 1:
                                            parts.append(flat[top : top + mz, left : left + ROWS])
                            low = s * hm + b * mz
                            tbuf[jx * nq + ql, low : low + mz, :] = jnp.concatenate(parts, 1)

        def store_modes(send):
            for jx in range(jxl):
                for ql in range(nq):
                    columns_of = []
                    for s in range(pd):
                        own = obuf[jx * nq + ql, s * hm : (s + 1) * hm, :]
                        if packed == 1:
                            columns_of.append(
                                jnp.concatenate(
                                    [
                                        own[b * mz : (b + 1) * mz, ri * ch : (ri + 1) * ch]
                                        for b in range(fold)
                                        for ri in range(2)
                                    ],
                                    0,
                                )
                            )
                        else:
                            for c in range(chunks):
                                columns_of.append(
                                    jnp.concatenate(
                                        [
                                            own[
                                                b * mz : (b + 1) * mz,
                                                ri * ch + (c * packed + gi) * ROWS : ri * ch + (c * packed + gi + 1) * ROWS,
                                            ]
                                            for gi in range(packed)
                                            for b in range(fold)
                                            for ri in range(2)
                                        ],
                                        0,
                                    )
                                )
                    back = jnp.concatenate(columns_of, 1).T.astype(BF16)
                    for s in range(pd):
                        for c in range(chunks):
                            low = (s * chunks + c) * ROWS
                            send[c, s, ql, jx * ROWS : (jx + 1) * ROWS, :] = back[low : low + ROWS, :]

        def each_mode(apply):
            def one(jq, carry):
                for r in range(hm):
                    own = tbuf[jq, pl.ds(r, pd, stride=hm), :]
                    obuf[jq, pl.ds(r, pd, stride=hm), :] = apply(jq * hm + r, own)
                return carry

            lax.fori_loop(0, jxl * nq, one, 0)

        def first(g, carry):
            def one(i, inner):
                x0 = i * batch
                for k in range(batch // PAIR):
                    load(field, fbuf, fsem, g, i * (batch // PAIR) + k).wait()
                for e in range(batch):
                    forward_z(
                        jnp.concatenate(
                            [fbuf[x0 + e, ys, cs, :].reshape(nyh * ROWS, nz) for ys, cs, _ in places(g)], 1
                        ),
                        e,
                    )
                forward_y(x0)
                return inner

            lax.fori_loop(0, batches, one, 0)
            forward_x(usend, g)

            @pl.when(g == 0)
            def _():
                pl.semaphore_wait(barrier, n - 1)

            start_sends(lambda t: usend.at[g, t], urecv, 0, g)
            return carry

        lax.fori_loop(0, chunks, first, 0)

        sign = jnp.where(lax.broadcasted_iota(jnp.int32, (1, 2 * ch), 1) < ch, -1.0, 1.0).astype(F32)

        def prepare(m, carry):
            own = w[m].astype(F32)
            wbig[m, :ch, :] = w[m]
            wbig[m, ch:, :] = (pltpu.roll(own, ch, 1) * sign).astype(BF16)
            return carry

        lax.fori_loop(0, w.shape[0], prepare, 0, unroll=4)
        fill(y_inv, y_back)
        fill(xi, x_back.at[my_p])
        mix(w_local[...].astype(F32).T, math.sqrt(0.5))

        def waits(recv, e):
            def one(g, carry):
                wait_recv(recv, e, g)
                return carry

            lax.fori_loop(0, chunks, one, 0)

        waits(urecv, 0)
        load_modes(urecv, False)

        def apply_one(m, own):
            ucat[m] = jnp.concatenate([own, pltpu.roll(own, ch, 1)], 0).astype(BF16)
            return mm(own.astype(BF16), wbig[m])

        each_mode(apply_one)
        store_modes(vsend)

        def send_v(g, carry):
            start_cast(vsend, vrecv, 0, g)
            return carry

        lax.fori_loop(0, chunks, send_v, 0)
        wait_sends(urecv, 0)

        def middle(g, carry):
            @pl.when(g == 0)
            def _():
                relay(vrecv, 0, g)

            wait_cast(vrecv, 0, g)
            inverse_x(vrecv, g)

            @pl.when(g < chunks - 1)
            def _():
                relay(vrecv, 0, g + 1)


            def one(i, inner):
                x0 = i * batch
                for k in range(batch // PAIR):
                    load(cot, cbuf, csem, g, i * (batch // PAIR) + k).wait()
                for k in range(0, batch, PAIR):
                    cstage[:, k * lanes : (k + PAIR) * lanes] = inverse_y(x0 + k)
                for e in range(batch):
                    grid = mm(cstage[:, e * lanes : (e + 1) * lanes], z_inv[...])
                    pieces = []
                    for ys, cs, left in places(g):
                        q = grid[:, left : left + nz].reshape(nyh, ROWS, nz) + fbuf[x0 + e, ys, cs, :].astype(F32)
                        slope = (cbuf[x0 + e, ys, cs, :].astype(F32) * twice_gelu_slope(q)).astype(BF16)
                        fbuf[x0 + e, ys, cs, :] = slope
                        pieces.append(slope.reshape(nyh * ROWS, nz))
                    forward_z(jnp.concatenate(pieces, 1), e)
                forward_y(x0)
                return inner

            lax.fori_loop(0, batches, one, 0)
            forward_x(usend, g)
            start_sends(lambda t: usend.at[g, t], grecv, 1, g)
            return carry

        lax.fori_loop(0, chunks, middle, 0)

        mix(w_local[...].astype(F32) * 0.5, 1.0)

        def spread_out(x):
            return pltpu.make_async_copy(fbuf.at[x], spread.at[x], osem.at[x])

        def put(x, carry):
            spread_out(x).start()
            return carry

        lax.fori_loop(0, xl, put, 0)

        waits(grecv, 1)
        load_modes(grecv, True)

        def adjoint_one(m, own):
            own = own.astype(BF16).astype(F32)
            gcat[m] = jnp.concatenate([own, pltpu.roll(own, ch, 1) * -sign], 0).astype(BF16)
            return lax.dot_general(
                own.astype(BF16), wbig[m], (((1,), (1,)), ((), ())), preferred_element_type=F32
            )

        each_mode(adjoint_one)
        store_modes(bsend)

        def send_b(g, carry):
            start_cast(bsend, brecv, 1, g)
            return carry

        lax.fori_loop(0, chunks, send_b, 0)

        def cols_out(g, x):
            return pltpu.make_async_copy(cols.at[g, x], columns.at[g, x], colsem.at[g, x])

        def last(g, carry):
            relay(brecv, 1, g)
            wait_cast(brecv, 1, g)
            inverse_x(brecv, g)

            def one(i, inner):
                for k in range(0, batch, PAIR):
                    x0 = i * batch + k
                    col = inverse_y(x0)
                    for e in range(PAIR):
                        cols[g, x0 + e] = col[:, e * lanes : (e + 1) * lanes]
                return inner

            lax.fori_loop(0, batches, one, 0)

            def out(x, inner):
                cols_out(g, x).start()
                return inner

            lax.fori_loop(0, xl, out, 0)
            return carry

        lax.fori_loop(0, chunks, last, 0)
        end_cast(vrecv, 0)
        wait_sends(grecv, 1)
        end_cast(brecv, 1)

        def finish(x, carry):
            spread_out(x).wait()
            for g in range(chunks):
                cols_out(g, x).wait()
            return carry

        lax.fori_loop(0, xl, finish, 0)

    return kernel


def make_last(fold, packed, chunks):
    def kernel(spread, columns, z_adj, ucat, gcat, grad, grad_w):
        xs, ny, ch, nz = spread.shape
        nyh = ny // fold
        for x in range(xs):
            for g in range(chunks):
                grid = mm(columns[g, x], z_adj[...])
                for gi in range(packed):
                    for h in range(fold):
                        left = (gi * fold + h) * nz
                        ys = slice(h * nyh, (h + 1) * nyh)
                        cs = slice((g * packed + gi) * ROWS, (g * packed + gi + 1) * ROWS)
                        value = grid[:, left : left + nz].reshape(nyh, ROWS, nz)
                        grad[x, ys, cs, :] = (value + spread[x, ys, cs, :].astype(F32)).astype(BF16)
        for m in range(grad_w.shape[0]):
            grad_w[m] = lax.dot_general(
                ucat[m], gcat[m], (((0,), (0,)), ((), ())), preferred_element_type=F32
            )[:ch]

    return kernel


def whole(array):
    return pl.BlockSpec(array.shape, lambda i, n=len(array.shape): (0,) * n)


def solution(mesh):
    pd, pp = mesh.shape["dp"], mesh.shape["pencil"]

    def body(field, cotangent, w_spec, w_local):
        sample, target = field[0], cotangent[0]
        xl, ny, ch, nz = sample.shape
        jxl, jyl, mz = w_spec.shape[:3]
        mx, my = jxl * pd, jyl * pp
        groups = ch // ROWS
        fold = math.gcd(jyl, groups)
        packed = groups // fold
        chunks = groups // packed
        lanes = groups * 2 * mz
        nq = jyl // fold
        n = pd * pp
        modes = jxl * jyl * mz
        pairs = xl // PAIR
        nyh = ny // fold
        t = make_tables(xl * pp, ny, nz, fold, packed, mx, my, mz, pp)
        weights = w_spec.reshape(modes, ch, 2 * ch)
        hbm = pl.BlockSpec(memory_space=pl.ANY)
        vmem = pl.BlockSpec(memory_space=pltpu.VMEM)
        names = ("z_fwd", "y_fwd", "r_fwd", "x_fwd", "x_inv", "turn", "r_inv", "y_inv", "z_inv", "scale")
        tables = [t[name] for name in names]
        table_specs = [vmem] * len(names)
        batch = math.gcd(xl, BATCH)
        block = (nq, jxl * ROWS, lanes)
        part = pltpu.VMEM((chunks, n) + block, BF16)
        mode_part = pltpu.VMEM((chunks, pd) + block, BF16)
        section = pltpu.VMEM((xl, my * ROWS, lanes), BF16)
        grid_buf = pltpu.VMEM(sample.shape, BF16)
        by_mode = pltpu.VMEM((jxl * nq, pd * fold * mz, 2 * ch), F32)
        dma = pltpu.SemaphoreType.DMA
        dims = (pd, pp, jxl, jyl, mz, fold, packed, chunks)
        cat = jax.ShapeDtypeStruct((modes, 2 * pd, 2 * ch), BF16)
        spread, columns, ucat, gcat = pl.pallas_call(
            make_main(dims),
            in_specs=[hbm, hbm, vmem, vmem] + table_specs,
            out_specs=[hbm, hbm, vmem, vmem],
            out_shape=[
                jax.ShapeDtypeStruct(sample.shape, BF16),
                jax.ShapeDtypeStruct((chunks, xl, nyh * ROWS, lanes), BF16),
                cat,
                cat,
            ],
            scratch_shapes=[
                grid_buf, grid_buf,
                pltpu.VMEM((chunks, xl, nyh * ROWS, lanes), BF16),
                section, section, section,
                part, mode_part, mode_part,
                part, part, part, part,
                pltpu.VMEM((modes, 2 * ch, 2 * ch), BF16),
                by_mode, by_mode,
                pltpu.VMEM((mx * ROWS, 2 * xl * ROWS), BF16),
                pltpu.VMEM((xl * ROWS, 2 * mx * ROWS), BF16),
                pltpu.VMEM((my * ROWS, 2 * nyh * ROWS), BF16),
                pltpu.VMEM((nyh * ROWS, 2 * my * ROWS), BF16),
                pltpu.VMEM((YB * ch, YB * ch), BF16),
                pltpu.VMEM((2 * nyh * ROWS, batch * lanes), BF16),
                pltpu.VMEM((nyh * ROWS, batch * lanes), BF16),
                dma((chunks, pairs)), dma((chunks, pairs)),
                dma((2, chunks)), dma((2, chunks)),
                dma((2, chunks)), dma((2, 2, chunks)), dma((2, chunks, max(pp // 2 - 1, 1))), dma((xl,)), dma((chunks, xl)),
            ],
            compiler_params=pltpu.CompilerParams(
                collective_id=0, has_side_effects=True, vmem_limit_bytes=VMEM
            ),
        )(sample, target, weights, w_local, *tables)

        rows = math.gcd(xl, LAST)
        steps = xl // rows
        per = modes // steps
        grad, grad_w = pl.pallas_call(
            make_last(fold, packed, chunks),
            grid=(steps,),
            in_specs=[
                pl.BlockSpec((rows, ny, ch, nz), lambda i: (i, 0, 0, 0)),
                pl.BlockSpec((chunks, rows, nyh * ROWS, lanes), lambda i: (0, i, 0, 0)),
                whole(t["z_adj"]),
                pl.BlockSpec((per, 2 * pd, 2 * ch), lambda i: (i, 0, 0)),
                pl.BlockSpec((per, 2 * pd, 2 * ch), lambda i: (i, 0, 0)),
            ],
            out_specs=[
                pl.BlockSpec((rows, ny, ch, nz), lambda i: (i, 0, 0, 0)),
                pl.BlockSpec((per, ch, 2 * ch), lambda i: (i, 0, 0)),
            ],
            out_shape=[
                jax.ShapeDtypeStruct(sample.shape, BF16),
                jax.ShapeDtypeStruct((modes, ch, 2 * ch), F32),
            ],
            compiler_params=pltpu.CompilerParams(
                dimension_semantics=("arbitrary",), vmem_limit_bytes=VMEM
            ),
        )(spread, columns, t["z_adj"], ucat, gcat)
        return grad[None], grad_w.reshape(w_spec.shape)

    grid_spec = P("dp", "pencil", None, None, None)
    return jax.shard_map(
        body,
        mesh=mesh,
        in_specs=(grid_spec, grid_spec, grid_spec, P()),
        out_specs=(grid_spec, grid_spec),
        check_vma=False,
    )
```
